128 devices in a mesh: gx: 8 (over y, core), yz: 16 (over x, z).
Axes of the slice: x: 4, y: 4, z: 4, core: 2. Of those that a mesh axis runs over, the one named last changes fastest.
Arguments:
- gas_state: float32 [5, 128, 256, 256], P(None, 'gx', 'yz'), may hold values from -6 to 6
- parcel_speed: float32 [8, 16, 128, 4, 3, 128], P('gx', 'yz'), may hold values from -6 to 6
- parcel_mass: float32 [8, 16, 128, 4, 128], P('gx', 'yz'), may hold values from 0.3 to 3
- offsets: float32 [8, 16, 128, 4, 3, 128], P('gx', 'yz'), may hold values from 0 to 1
- cell_base: int32 [8, 16, 128, 4, 3, 128], P('gx', 'yz'), may hold values from 0 to 6, as said below
- block_tile: int32 [8, 16, 128, 4], P('gx', 'yz'), may hold values from 0 to 511
- block_count: int32 [8, 16, 128], P('gx', 'yz'), may hold values from 0 to 4, as said below
Outputs:
- gas_next: float32 [5, 128, 256, 256], P(None, 'gx', 'yz')
- speed_next: float32 [8, 16, 128, 4, 3, 128], P('gx', 'yz')
- mass_next: float32 [8, 16, 128, 4, 128], P('gx', 'yz')
The draws below stay inside these ranges and needn't reach their ends.
Inputs may be any that keep to these rules, and one draw needn't show every extreme that they name: `block_count`: A device's live blocks for an owner are its first ones; in every draw some owner receives 4 live blocks from every device. `cell_base`: component 0, 1, 2 is at most 2, 2, 6, so that the base cell and the next cell along each dimension lie in the tile.
All inputs are finite; a program needn't handle non-finite values.
Results may differ from the reference program's by a relative error of at most 0.0003.
Values sent between devices are 32-bit elements; how exact they have to be, the bound alone decides.
A program may use at most 128 MiB of HBM per device.

```python
import math
import jax
import jax.numpy as jnp
from jax import lax

CX = 16
CY = 16
NZ = 256
CAP = 4
PB = 128
TILE_X = 4
TILE_Y = 4
TILE_Z = 8
NX = 128
NY = 256
TILES_DEV = 512
N_GX = 8
N_YZ = 16
DEVICES = 128


def draw_cell_base(key, part):
    folded = jax.random.fold_in(key, 11)
    raw = jax.random.randint(folded, (N_GX, N_YZ, DEVICES, CAP, 3, PB), 0, 1 << 20, dtype=jnp.int32)
    limits = jnp.array([TILE_X - 1, TILE_Y - 1, TILE_Z - 1], dtype=jnp.int32).reshape(3, 1)
    return raw % limits


def draw_block_count(key, part):
    folded = jax.random.fold_in(key, 23)
    first_key, second_key = jax.random.split(folded)
    owners = jnp.arange(DEVICES, dtype=jnp.int32)
    row_index = owners // N_YZ
    col_index = owners % N_YZ
    heat = N_GX - row_index + (N_YZ // 2 - jnp.abs(col_index - N_YZ // 2))
    ceiling = N_GX + N_YZ // 2
    raw = jax.random.randint(first_key, (N_GX, N_YZ, DEVICES), 0, 2 * CAP + 2, dtype=jnp.int32)
    counted = jnp.minimum(CAP, raw * heat // ceiling)
    chosen = jax.random.randint(second_key, (), 0, DEVICES, dtype=jnp.int32)
    return jnp.where(owners == chosen, CAP, counted).astype(jnp.int32)


def with_ends(result, stream_key, least, top_value):
    place = [jax.random.randint(jax.random.fold_in(stream_key, axis), (), 0, length) for axis, length in enumerate(result.shape)]
    main_axis = result.shape.index(max(result.shape))
    next_to = place[:main_axis] + [(place[main_axis] + 1) % result.shape[main_axis]] + place[main_axis + 1:]
    return result.at[tuple(place)].set(least).at[tuple(next_to)].set(top_value)


def shard_levels(own_key, shape, cuts, smallest, top_value):
    loudness, own = 1.0, jax.random.fold_in(own_key, 6)
    for dim, blocks in cuts:
        steps = jnp.exp(jax.random.uniform(jax.random.fold_in(own, dim), (blocks,), jnp.float32, smallest / len(cuts), top_value / len(cuts)))
        loudness = loudness * jnp.repeat(steps, shape[dim] // blocks).reshape([-1 if axis == dim else 1 for axis in range(len(shape))])
    return loudness


def bell_draw(stream_key, dims, deviation, limit, cuts=(), kind=jnp.bfloat16):
    result = deviation * jax.random.normal(stream_key, dims, jnp.float32)
    if cuts:
        result = result * shard_levels(stream_key, dims, cuts, -0.22, 0.18)
    return jnp.clip(result, -limit, limit).astype(kind)


def setup_inputs(seed: int = 0) -> dict:
    streams_of = jax.random.split(jax.random.key(seed), 8)
    gas_state = bell_draw(streams_of[0], (5, NX, NY, NZ), 1.0, 6.0, ((1, 8), (2, 16)), jnp.float32)
    parcel_speed = bell_draw(streams_of[1], (N_GX, N_YZ, DEVICES, CAP, 3, PB), 1.0, 6.0, ((0, 8), (1, 16)), jnp.float32)
    parcel_mass = jnp.clip(jnp.exp(math.log(3.0) - 2.3025851 * jax.random.uniform(streams_of[2], (N_GX, N_YZ, DEVICES, CAP, PB), jnp.float32) ** shard_levels(streams_of[2], (N_GX, N_YZ, DEVICES, CAP, PB), ((0, 8), (1, 16)), -0.2, 0.2)), 0.3, 3.0)
    offsets = jnp.clip(1.0 * jax.random.uniform(streams_of[3], (N_GX, N_YZ, DEVICES, CAP, 3, PB), jnp.float32) ** shard_levels(streams_of[3], (N_GX, N_YZ, DEVICES, CAP, 3, PB), ((0, 8), (1, 16)), -0.2, 0.2), 0.0, 1.0)
    cell_base = draw_cell_base(jax.random.fold_in(streams_of[7], 71), 0)
    block_tile = with_ends(jax.random.randint(streams_of[5], (N_GX, N_YZ, DEVICES, CAP), 0, TILES_DEV), jax.random.fold_in(streams_of[5], 1), 0, TILES_DEV - 1).astype(jnp.int32)
    block_count = draw_block_count(jax.random.fold_in(streams_of[7], 71), 0)
    return dict(gas_state=gas_state, parcel_speed=parcel_speed, parcel_mass=parcel_mass, offsets=offsets, cell_base=cell_base, block_tile=block_tile, block_count=block_count)


DIFFUSION = 0.1
CELL_MASS = 4.0
DRAG_RATE = 0.5
EVAPORATION = 0.3
LATENT_HEAT = 2.0


def split_tiles(block):
    fields, extent_x, extent_y, extent_z = block.shape
    grid = block.reshape(fields, extent_x // TILE_X, TILE_X, extent_y // TILE_Y, TILE_Y, extent_z // TILE_Z, TILE_Z)
    grid = grid.transpose(1, 3, 5, 0, 2, 4, 6)
    return grid.reshape(-1, fields, TILE_X * TILE_Y * TILE_Z)


def join_tiles(tile_data, extent_x, extent_y, extent_z):
    fields = tile_data.shape[1]
    grid = tile_data.reshape(extent_x // TILE_X, extent_y // TILE_Y, extent_z // TILE_Z, fields, TILE_X, TILE_Y, TILE_Z)
    return grid.transpose(3, 0, 4, 1, 5, 2, 6).reshape(fields, extent_x, extent_y, extent_z)


def laplace(padded):
    framed = jnp.pad(padded, ((0, 0), (0, 0), (0, 0), (1, 1)))
    centre = framed[:, 1:-1, 1:-1, 1:-1]
    beside_all = framed[:, 2:, 1:-1, 1:-1] + framed[:, :-2, 1:-1, 1:-1]
    beside_all = beside_all + framed[:, 1:-1, 2:, 1:-1] + framed[:, 1:-1, :-2, 1:-1]
    beside_all = beside_all + framed[:, 1:-1, 1:-1, 2:] + framed[:, 1:-1, 1:-1, :-2]
    return beside_all - 6.0 * centre


def weights_along(fraction, base_cell, extent):
    positions = jnp.arange(extent, dtype=jnp.int32)
    lower_hit = (base_cell[..., None] == positions).astype(jnp.float32)
    upper_hit = (base_cell[..., None] + 1 == positions).astype(jnp.float32)
    return (1.0 - fraction)[..., None] * lower_hit + fraction[..., None] * upper_hit


def parcel_update(tile_data, velocity, shifts, cells, mass_old, live):
    along_x = weights_along(shifts[:, 0], cells[:, 0], TILE_X)
    along_y = weights_along(shifts[:, 1], cells[:, 1], TILE_Y)
    along_z = weights_along(shifts[:, 2], cells[:, 2], TILE_Z)
    stencil = along_x[:, :, :, None, None] * along_y[:, :, None, :, None] * along_z[:, :, None, None, :]
    stencil = stencil.reshape(mass_old.shape + (TILE_X * TILE_Y * TILE_Z,))
    sampled = jnp.einsum("scq,spq->scp", tile_data, stencil, precision=lax.Precision.HIGHEST)
    radius = jnp.cbrt(mass_old)
    factor = DRAG_RATE / (radius * radius)
    alive = live > 0.5
    moved = (velocity + factor[:, None, :] * sampled[:, 0:3]) / (1.0 + factor[:, None, :])
    velocity_new = jnp.where(alive[:, None, None], moved, velocity)
    evap_loss = EVAPORATION * jax.nn.softplus(sampled[:, 3] - sampled[:, 4]) / radius
    mass_new = jnp.where(alive[:, None], mass_old / (1.0 + evap_loss), mass_old)
    vapour = mass_old - mass_new
    momentum = mass_old[:, None, :] * (velocity - velocity_new) + vapour[:, None, :] * velocity_new
    source = jnp.concatenate([momentum, -LATENT_HEAT * vapour[:, None, :], vapour[:, None, :]], axis=1)
    source = source * live[:, None, None]
    deposit = jnp.einsum("scp,spq->scq", source, stencil, precision=lax.Precision.HIGHEST)
    return velocity_new, mass_new, deposit


def reference(gas_state, parcel_speed, parcel_mass, offsets, cell_base, block_tile, block_count):
    blocks = gas_state.reshape(5, N_GX, CX, N_YZ, CY, NZ).transpose(1, 3, 0, 2, 4, 5).reshape(DEVICES, 5, CX, CY, NZ)
    all_tiles = jax.vmap(split_tiles)(blocks)
    owners = jnp.arange(DEVICES, dtype=jnp.int32)[:, None]
    slot_total = DEVICES * CAP

    def per_source(packed):
        velocity, mass_old, shifts, cells, tile_index, counted = packed
        chosen = all_tiles[owners, tile_index]
        live = (jnp.arange(CAP, dtype=jnp.int32)[None, :] < counted[:, None]).astype(jnp.float32)
        velocity_new, mass_new, deposit = parcel_update(
            chosen.reshape((slot_total,) + chosen.shape[2:]),
            velocity.reshape((slot_total,) + velocity.shape[2:]),
            shifts.reshape((slot_total,) + shifts.shape[2:]),
            cells.reshape((slot_total,) + cells.shape[2:]),
            mass_old.reshape((slot_total,) + mass_old.shape[2:]),
            live.reshape(slot_total))
        return velocity_new.reshape(velocity.shape), mass_new.reshape(mass_old.shape), deposit.reshape(chosen.shape)

    block_index = block_tile.reshape(DEVICES, DEVICES, CAP)
    packed = (parcel_speed.reshape(DEVICES, DEVICES, CAP, 3, PB),
              parcel_mass.reshape(DEVICES, DEVICES, CAP, PB),
              offsets.reshape(DEVICES, DEVICES, CAP, 3, PB),
              cell_base.reshape(DEVICES, DEVICES, CAP, 3, PB),
              block_index,
              block_count.reshape(DEVICES, DEVICES))
    speed_out, mass_out, deposits = lax.map(per_source, packed)
    targets = owners[None, :, :] * TILES_DEV + block_index
    summed = jax.ops.segment_sum(deposits.reshape(-1, 5, TILE_X * TILE_Y * TILE_Z), targets.reshape(-1),
                                 num_segments=DEVICES * TILES_DEV)

    def join_owner(tile_data):
        return join_tiles(tile_data, CX, CY, NZ)

    source_blocks = jax.vmap(join_owner)(summed.reshape(DEVICES, TILES_DEV, 5, -1))
    source_field = source_blocks.reshape(N_GX, N_YZ, 5, CX, CY, NZ).transpose(2, 0, 3, 1, 4, 5).reshape(5, NX, NY, NZ)
    padded = jnp.pad(gas_state, ((0, 0), (1, 1), (1, 1), (0, 0)))
    gas_next = gas_state + DIFFUSION * laplace(padded) + source_field / CELL_MASS
    return gas_next, speed_out.reshape(parcel_speed.shape), mass_out.reshape(parcel_mass.shape)
```

```python
import functools

import jax
import jax.numpy as jnp
from jax import lax
from jax.experimental import pallas as pl
from jax.experimental.pallas import tpu as pltpu
from jax.sharding import PartitionSpec as P

F32 = jnp.float32
BF16 = jnp.bfloat16
I32 = jnp.int32

DIFFUSION = 0.1
CELL_MASS = 4.0
DRAG_RATE = 0.5
EVAPORATION = 0.3
LATENT_HEAT = 2.0

CORNERS = tuple((u, v, w) for u in (0, 1) for v in (0, 1) for w in (0, 1))
SHIFTS = tuple(u * 32 + v * 8 + w for u, v, w in CORNERS)


def lanes():
    return lax.broadcasted_iota(I32, (8, 128), 1)


def rows():
    return lax.broadcasted_iota(I32, (8, 128), 0)


def chunk_swaps():
    row, lane = rows(), lanes()
    half, chunk, rest = lane // 64, (lane // 8) % 8, lane % 8
    first = half * 64 + ((chunk - row) % 8) * 8 + rest
    second = (chunk - row) % 8
    third = half * 64 + ((chunk + row) % 8) * 8 + rest
    return first, second, third


def transpose_chunks(block, swaps):
    first, second, third = swaps
    block = jnp.take_along_axis(block, first, axis=1)
    block = jnp.take_along_axis(block, second, axis=0)
    return jnp.take_along_axis(block, third, axis=1)


def swap_halves(a, b, axis):
    size = a.shape[axis] // 2
    low = (lanes() < 64) if axis == 1 else (rows() < 4)
    crossed = pltpu.roll(jnp.where(low, b, a), size, axis)
    return jnp.where(low, a, crossed), jnp.where(low, crossed, b)


def grid_to_tiles(blocks, swaps):
    pairs = [swap_halves(blocks[k], blocks[2 + k], 1) for k in (0, 1)]
    out = []
    for z in (0, 1):
        halves = swap_halves(pairs[0][z], pairs[1][z], 0)
        out.append([transpose_chunks(one, swaps) for one in halves])
    return out


def tiles_to_grid(tiles, swaps):
    pairs = []
    for z in (0, 1):
        a, b = (transpose_chunks(one, swaps) for one in tiles[z])
        pairs.append(swap_halves(a, b, 0))
    blocks = [None] * 4
    for k in (0, 1):
        blocks[k], blocks[2 + k] = swap_halves(pairs[0][k], pairs[1][k], 1)
    return blocks


def table_kernel(gas_ref, table_ref):
    swaps = chunk_swaps()

    def step(n, carry):
        a, yo = n // 2, n % 2
        y0 = pl.multiple_of(yo * 8, 8)
        for h in (0, 1):
            for f in range(4):
                blocks = []
                for u in range(4):
                    part = gas_ref[f, a * 4 + u, pl.ds(y0, 8), pl.ds(h * 128, 128)]
                    if f == 3:
                        part = part - gas_ref[4, a * 4 + u, pl.ds(y0, 8), pl.ds(h * 128, 128)]
                    blocks.append(part)
                tiles = grid_to_tiles(blocks, swaps)
                for z in (0, 1):
                    for bh in (0, 1):
                        t0 = (a * 4 + yo * 2 + bh) * 32 + (h * 2 + z) * 8
                        table_ref[pl.ds(t0 * 4 + f, 8, stride=4), :] = tiles[z][bh]
        return carry

    lax.fori_loop(0, 8, step, 0)


def gather_kernel(index_ref, table_ref, out_ref):
    def step(n, carry):
        for k in range(16):
            s = n * 16 + k
            out_ref[s] = table_ref[index_ref[s]]
        return carry

    lax.fori_loop(0, out_ref.shape[0] // 16, step, 0)


def split_three(ref, g):
    low = rows() < 4
    v0, v1, v2 = (ref[pl.ds(pl.multiple_of(g * 24 + 8 * n, 8), 8), :] for n in range(3))
    middle = pltpu.roll(jnp.where(low, v2, v0), 4, 0)
    return jnp.where(low, v0, v1), middle, jnp.where(low, v1, v2)


def join_three(ref, g, f0, f1, f2):
    low = rows() < 4
    middle = pltpu.roll(f1, 4, 0)
    out = (jnp.where(low, f0, middle), jnp.where(low, f2, f0), jnp.where(low, middle, f2))
    for n in range(3):
        ref[pl.ds(pl.multiple_of(g * 24 + 8 * n, 8), 8), :] = out[n]


def parcels(g, count_ref, tiles_ref, speed_ref, mass_ref, offset_ref, cell_ref, speed_out, mass_out, lhs_ref, q_ref):
    low = rows() < 4
    cx, cy, cz = split_three(cell_ref, g)
    ox, oy, oz = split_three(offset_ref, g)
    speed = split_three(speed_ref, g)
    mass = mass_ref[pl.ds(pl.multiple_of(g * 8, 8), 8), :]
    q = cx * 32 + cy * 8 + cz
    wx, wy, wz = ((1.0 - o, o) for o in (ox, oy, oz))
    weights = []
    for u in (0, 1):
        for v in (0, 1):
            both = wx[u] * wy[v]
            weights += [both * wz[0], both * wz[1]]
    index = [q + shift for shift in SHIFTS]
    sampled = []
    for f in range(4):
        tile = tiles_ref[pl.ds(g * 32 + f, 8, stride=4), :]
        total = None
        for c in range(8):
            term = jnp.take_along_axis(tile, index[c], axis=1) * weights[c]
            total = term if total is None else total + term
        sampled.append(total)
    log_radius = jnp.log(mass) * (1.0 / 3.0)
    inverse_radius = jnp.exp(-log_radius)
    drag = DRAG_RATE * inverse_radius * inverse_radius
    live = (rows() % 4) < jnp.where(low, count_ref[2 * g], count_ref[2 * g + 1])
    scale = 1.0 / (1.0 + drag)
    gap = sampled[3]
    softplus = jnp.maximum(gap, 0.0) + jnp.log(1.0 + jnp.exp(-jnp.abs(gap)))
    mass_new = mass / (1.0 + EVAPORATION * softplus * inverse_radius)
    mass_new = jnp.where(live, mass_new, mass)
    vapour = mass - mass_new
    speed_new, source = [], []
    for f in range(3):
        moved = jnp.where(live, (speed[f] + drag * sampled[f]) * scale, speed[f])
        speed_new.append(moved)
        source.append(mass * (speed[f] - moved) + vapour * moved)
    source.append(vapour)
    join_three(speed_out, g, *speed_new)
    mass_out[pl.ds(pl.multiple_of(g * 8, 8), 8), :] = mass_new
    for f in range(4):
        value = jnp.where(live, source[f], 0.0)
        for c in range(8):
            lhs_ref[pl.ds(c * 32 + f, 8, stride=4), :] = value * weights[c]
    q_ref[...] = q


def deposits(g, lhs_ref, q_ref, out_ref):
    entry = lax.broadcasted_iota(I32, (128, 128), 0)
    first = lax.broadcasted_iota(I32, (64, 128), 0) % 8 < 4
    keep = jnp.where(first, 1.0, 0.0).astype(BF16)
    drop = jnp.where(first, 0.0, 1.0).astype(BF16)
    for j in range(4):
        left = jnp.concatenate([lhs_ref[pl.ds(c * 32 + j * 8, 8), :] for c in range(8)], axis=0)
        high = left.astype(BF16)
        rest = (left - high.astype(F32)).astype(BF16)
        left = jnp.concatenate(
            [
                jnp.concatenate([high * keep, high * drop], axis=1),
                jnp.concatenate([rest * keep, rest * drop], axis=1),
            ],
            axis=0,
        )
        hits = []
        for k in (0, 1):
            at = jnp.broadcast_to(q_ref[pl.ds(2 * j + k, 1), :], (128, 128))
            hits.append(jnp.where(at == entry, 1.0, 0.0).astype(BF16))
        right = jnp.concatenate(hits, axis=1)
        both = lax.dot_general(left, right, (((1,), (1,)), ((), ())), preferred_element_type=F32)
        both = both[:64] + both[64:]
        total = both[:8]
        for c in range(1, 8):
            total = total + pltpu.roll(both[c * 8 : c * 8 + 8], SHIFTS[c], 1)
        out_ref[pl.ds(pl.multiple_of(g * 32 + j * 8, 8), 8), :] = total


def parcel_kernel(count_ref, tiles_ref, speed_ref, mass_ref, offset_ref, cell_ref, speed_out, mass_out, out_ref, lhs_ref, q_ref):
    groups = mass_ref.shape[0] // 8

    def first(g):
        parcels(g, count_ref, tiles_ref, speed_ref, mass_ref, offset_ref, cell_ref, speed_out, mass_out, lhs_ref, q_ref)

    def step(g, carry):
        deposits(g - 1, lhs_ref, q_ref, out_ref)
        first(g)
        return carry

    first(0)
    lax.fori_loop(1, groups, step, 0)
    deposits(groups - 1, lhs_ref, q_ref, out_ref)


def spread(plane_ref, f, x, xs, halos):
    xlo, xhi, ylo, yhi = halos
    value = plane_ref[f, x]
    row = lax.broadcasted_iota(I32, value.shape, 0)
    lane = lax.broadcasted_iota(I32, value.shape, 1)
    ny, nz = value.shape
    below = xlo[f] if x == 0 else plane_ref[f, x - 1]
    above = xhi[f] if x == xs - 1 else plane_ref[f, x + 1]
    total = below + above
    total = total + jnp.where(row == 0, ylo[f, x : x + 1, :], pltpu.roll(value, 1, 0))
    total = total + jnp.where(row == ny - 1, yhi[f, x : x + 1, :], pltpu.roll(value, ny - 1, 0))
    total = total + jnp.where(lane == 0, 0.0, pltpu.roll(value, 1, 1))
    total = total + jnp.where(lane == nz - 1, 0.0, pltpu.roll(value, nz - 1, 1))
    return value + DIFFUSION * (total - 6.0 * value)


def diffuse_kernel(gas_ref, xlo, xhi, ylo, yhi, out_ref):
    xs = gas_ref.shape[1]

    def step(f, carry):
        for x in range(xs):
            out_ref[f, x] = spread(gas_ref, f, x, xs, (xlo, xhi, ylo, yhi))
        return carry

    lax.fori_loop(0, gas_ref.shape[0], step, 0)


def scatter_kernel(index_ref, arrived_ref, *sum_refs):
    for ref in sum_refs:
        ref[...] = jnp.zeros_like(ref)

    def step(n, carry):
        for k in range(4):
            for m in range(4):
                s = n * 16 + k * 4 + m
                t = index_ref[s]
                sum_refs[m][t] += arrived_ref[s]
        return carry

    lax.fori_loop(0, arrived_ref.shape[0] // 16, step, 0)


def join_kernel(base_ref, s0, s1, s2, s3, out_ref):
    swaps = chunk_swaps()

    def step(n, carry):
        a, yo = n // 2, n % 2
        y0 = pl.multiple_of(yo * 8, 8)
        for h in (0, 1):
            for f in range(4):
                tiles = []
                for z in (0, 1):
                    tiles.append([])
                    for bh in (0, 1):
                        t0 = (a * 4 + yo * 2 + bh) * 32 + (h * 2 + z) * 8
                        at = pl.ds(t0 * 4 + f, 8, stride=4)
                        tiles[z].append((s0[at, :] + s1[at, :]) + (s2[at, :] + s3[at, :]))
                blocks = tiles_to_grid(tiles, swaps)
                for u in range(4):
                    at = (a * 4 + u, pl.ds(y0, 8), pl.ds(h * 128, 128))
                    add = blocks[u] * (1.0 / CELL_MASS)
                    if f < 3:
                        out_ref[f, *at] = base_ref[f, *at] + add
                    else:
                        out_ref[3, *at] = base_ref[3, *at] - LATENT_HEAT * add
                        out_ref[4, *at] = base_ref[4, *at] + add
        return carry

    lax.fori_loop(0, 8, step, 0)


VMEM = pl.BlockSpec(memory_space=pltpu.VMEM)
SMEM = pl.BlockSpec(memory_space=pltpu.SMEM)


def call(kernel, name, out, in_specs, scratch=()):
    return pl.pallas_call(
        kernel,
        name=name,
        out_shape=out,
        in_specs=in_specs,
        out_specs=jax.tree.map(lambda _: VMEM, out),
        scratch_shapes=scratch,
        compiler_params=pltpu.CompilerParams(vmem_limit_bytes=48 * 1024 * 1024),
    )


def array(*shape):
    return jax.ShapeDtypeStruct(shape, F32)


def shards(gas_state, parcel_speed, parcel_mass, offsets, cell_base, block_tile, block_count):
    fields, xs, ys, zs = gas_state.shape
    devices, capacity = block_tile.shape[2:]
    slots = devices * capacity
    tiles = xs * ys * zs // 128

    def three(value):
        value = value.reshape(devices, capacity, 3, 128).transpose(0, 2, 1, 3)
        return value.reshape(slots * 3, 128)

    index = block_tile.reshape(devices, capacity)
    wanted = lax.all_to_all(index, ("gx", "yz"), split_axis=0, concat_axis=0, tiled=True).reshape(slots)
    table = call(table_kernel, "table", array(tiles * 4, 128), [VMEM])(gas_state)

    def edges(axis, dim):
        count, length = lax.axis_size(axis), gas_state.shape[dim]
        up = [(i, i + 1) for i in range(count - 1)]
        last = lax.slice_in_dim(gas_state, length - 1, length, axis=dim)
        initial = lax.slice_in_dim(gas_state, 0, 1, axis=dim)
        return (
            jnp.squeeze(lax.ppermute(last, axis, up), dim),
            jnp.squeeze(lax.ppermute(initial, axis, [(b, a) for a, b in up]), dim),
        )

    halos = edges("gx", 1) + edges("yz", 2)
    send = call(gather_kernel, "gather", array(slots, 4, 128), [SMEM, VMEM])(wanted, table.reshape(tiles, 4, 128))
    fetched = lax.all_to_all(send, ("gx", "yz"), split_axis=0, concat_axis=0, tiled=True)
    base = call(diffuse_kernel, "diffuse", array(*gas_state.shape), [VMEM] * 5)(gas_state, *halos)
    speed_next, mass_next, deposit = call(
        parcel_kernel,
        "parcels",
        (array(slots * 3, 128), array(slots, 128), array(slots * 4, 128)),
        [SMEM] + [VMEM] * 5,
        [pltpu.VMEM((256, 128), F32), pltpu.VMEM((8, 128), I32)],
    )(
        block_count.reshape(devices),
        fetched.reshape(slots * 4, 128),
        three(parcel_speed),
        parcel_mass.reshape(slots, 128),
        three(offsets),
        three(cell_base),
    )
    arrived = lax.all_to_all(deposit.reshape(slots, 4, 128), ("gx", "yz"), split_axis=0, concat_axis=0, tiled=True)
    sums = call(scatter_kernel, "scatter", (array(tiles, 4, 128),) * 4, [SMEM, VMEM])(wanted, arrived)
    gas_next = call(join_kernel, "join", array(*gas_state.shape), [VMEM] * 5)(
        base, *(one.reshape(tiles * 4, 128) for one in sums)
    )
    speed_next = speed_next.reshape(devices, 3, capacity, 128).transpose(0, 2, 1, 3)
    return gas_next, speed_next.reshape(parcel_speed.shape), mass_next.reshape(parcel_mass.shape)


def solution(mesh):
    in_specs = (
        P(None, "gx", "yz", None),
        P("gx", "yz", None, None, None, None),
        P("gx", "yz", None, None, None),
        P("gx", "yz", None, None, None, None),
        P("gx", "yz", None, None, None, None),
        P("gx", "yz", None, None),
        P("gx", "yz", None),
    )
    out_specs = (
        P(None, "gx", "yz", None),
        P("gx", "yz", None, None, None, None),
        P("gx", "yz", None, None, None),
    )
    return jax.shard_map(shards, mesh=mesh, in_specs=in_specs, out_specs=out_specs, check_vma=False)
```

```python
import functools

import jax
import jax.numpy as jnp
from jax import lax
from jax.experimental import pallas as pl
from jax.experimental.pallas import tpu as pltpu
from jax.sharding import PartitionSpec as P

F32 = jnp.float32
BF16 = jnp.bfloat16
I32 = jnp.int32
MESH = pl.DeviceIdType.MESH

DIFFUSION = 0.1
CELL_MASS = 4.0
DRAG_RATE = 0.5
EVAPORATION = 0.3
LATENT_HEAT = 2.0

SHIFTS = (0, 1, 8, 9, 32, 33, 40, 41)

DEVICES = 128
SLOTS = 512
COLUMNS = 16
HERE = 4


def lanes():
    return lax.broadcasted_iota(I32, (8, 128), 1)


def rows():
    return lax.broadcasted_iota(I32, (8, 128), 0)


def chunk_swaps():
    row, lane = rows(), lanes()
    half, chunk, rest = lane // 64, (lane // 8) % 8, lane % 8
    first = half * 64 + ((chunk - row) % 8) * 8 + rest
    second = (chunk - row) % 8
    third = half * 64 + ((chunk + row) % 8) * 8 + rest
    return first, second, third


def transpose_chunks(block, swaps):
    first, second, third = swaps
    block = jnp.take_along_axis(block, first, axis=1)
    block = jnp.take_along_axis(block, second, axis=0)
    return jnp.take_along_axis(block, third, axis=1)


def swap_halves(a, b, axis):
    size = a.shape[axis] // 2
    low = (lanes() < 64) if axis == 1 else (rows() < 4)
    crossed = pltpu.roll(jnp.where(low, b, a), size, axis)
    return jnp.where(low, a, crossed), jnp.where(low, crossed, b)


def grid_to_tiles(blocks, swaps):
    pairs = [swap_halves(blocks[k], blocks[2 + k], 1) for k in (0, 1)]
    out = []
    for z in (0, 1):
        halves = swap_halves(pairs[0][z], pairs[1][z], 0)
        out.append([transpose_chunks(one, swaps) for one in halves])
    return out


def tiles_to_grid(tiles, swaps):
    pairs = []
    for z in (0, 1):
        a, b = (transpose_chunks(one, swaps) for one in tiles[z])
        pairs.append(swap_halves(a, b, 0))
    blocks = [None] * 4
    for k in (0, 1):
        blocks[k], blocks[2 + k] = swap_halves(pairs[0][k], pairs[1][k], 1)
    return blocks


def make_table(gas_ref, table_ref):
    swaps = chunk_swaps()
    flat_ref = table_ref.reshape(SLOTS * 4, 128)

    def step(n, carry):
        a, yo = n // 2, n % 2
        y0 = pl.multiple_of(yo * 8, 8)
        for h in (0, 1):
            for f in range(4):
                blocks = []
                for u in range(4):
                    part = gas_ref[f, a * 4 + u, pl.ds(y0, 8), pl.ds(h * 128, 128)]
                    if f == 3:
                        part = part - gas_ref[4, a * 4 + u, pl.ds(y0, 8), pl.ds(h * 128, 128)]
                    blocks.append(part)
                tiles = grid_to_tiles(blocks, swaps)
                for z in (0, 1):
                    for bh in (0, 1):
                        t0 = (a * 4 + yo * 2 + bh) * 32 + (h * 2 + z) * 8
                        flat_ref[pl.ds(t0 * 4 + f, 8, stride=4), :] = tiles[z][bh]
        return carry

    lax.fori_loop(0, 8, step, 0)


def split_three(ref, g):
    low = rows() < 4
    v0, v1, v2 = (ref[pl.ds(pl.multiple_of(g * 24 + 8 * n, 8), 8), :] for n in range(3))
    middle = pltpu.roll(jnp.where(low, v2, v0), 4, 0)
    return jnp.where(low, v0, v1), middle, jnp.where(low, v1, v2)


def join_three(ref, g, f0, f1, f2):
    low = rows() < 4
    middle = pltpu.roll(f1, 4, 0)
    out = (jnp.where(low, f0, middle), jnp.where(low, f2, f0), jnp.where(low, middle, f2))
    for n in range(3):
        ref[pl.ds(pl.multiple_of(g * 24 + 8 * n, 8), 8), :] = out[n]


def parcels(g, count_ref, tiles_ref, speed_ref, mass_ref, offset_ref, cell_ref, speed_out, mass_out, lhs_ref, q_ref):
    low = rows() < 4
    cx, cy, cz = split_three(cell_ref, g)
    ox, oy, oz = split_three(offset_ref, g)
    speed = split_three(speed_ref, g)
    mass = mass_ref[pl.ds(pl.multiple_of(g * 8, 8), 8), :]
    q = cx * 32 + cy * 8 + cz
    wx, wy, wz = ((1.0 - o, o) for o in (ox, oy, oz))
    weights = []
    for u in (0, 1):
        for v in (0, 1):
            both = wx[u] * wy[v]
            weights += [both * wz[0], both * wz[1]]
    index = [q + shift for shift in SHIFTS]
    sampled = []
    for f in range(4):
        tile = tiles_ref[pl.ds(g * 32 + f, 8, stride=4), :]
        total = None
        for c in range(8):
            term = jnp.take_along_axis(tile, index[c], axis=1) * weights[c]
            total = term if total is None else total + term
        sampled.append(total)
    log_radius = jnp.log(mass) * (1.0 / 3.0)
    inverse_radius = jnp.exp(-log_radius)
    drag = DRAG_RATE * inverse_radius * inverse_radius
    live = (rows() % 4) < jnp.where(low, count_ref[2 * g], count_ref[2 * g + 1])
    scale = 1.0 / (1.0 + drag)
    gap = sampled[3]
    softplus = jnp.maximum(gap, 0.0) + jnp.log(1.0 + jnp.exp(-jnp.abs(gap)))
    mass_new = mass / (1.0 + EVAPORATION * softplus * inverse_radius)
    mass_new = jnp.where(live, mass_new, mass)
    vapour = mass - mass_new
    speed_new, source = [], []
    for f in range(3):
        moved = jnp.where(live, (speed[f] + drag * sampled[f]) * scale, speed[f])
        speed_new.append(moved)
        source.append(mass * (speed[f] - moved) + vapour * moved)
    source.append(vapour)
    join_three(speed_out, g, *speed_new)
    mass_out[pl.ds(pl.multiple_of(g * 8, 8), 8), :] = mass_new
    for f in range(4):
        value = jnp.where(live, source[f], 0.0)
        for c in range(8):
            lhs_ref[pl.ds(c * 32 + f, 8, stride=4), :] = value * weights[c]
    q_ref[...] = q


def deposits(g, lhs_ref, q_ref, out_ref):
    entry = lax.broadcasted_iota(I32, (128, 128), 0)
    first = lax.broadcasted_iota(I32, (64, 128), 0) % 8 < 4
    keep = jnp.where(first, 1.0, 0.0).astype(BF16)
    drop = jnp.where(first, 0.0, 1.0).astype(BF16)
    for j in range(4):
        left = jnp.concatenate([lhs_ref[pl.ds(c * 32 + j * 8, 8), :] for c in range(8)], axis=0)
        high = left.astype(BF16)
        rest = (left - high.astype(F32)).astype(BF16)
        left = jnp.concatenate(
            [
                jnp.concatenate([high * keep, high * drop], axis=1),
                jnp.concatenate([rest * keep, rest * drop], axis=1),
            ],
            axis=0,
        )
        hits = []
        for k in (0, 1):
            at = jnp.broadcast_to(q_ref[pl.ds(2 * j + k, 1), :], (128, 128))
            hits.append(jnp.where(at == entry, 1.0, 0.0).astype(BF16))
        right = jnp.concatenate(hits, axis=1)
        both = lax.dot_general(left, right, (((1,), (1,)), ((), ())), preferred_element_type=F32)
        both = both[:64] + both[64:]
        total = both[:8]
        for c in range(1, 8):
            total = total + pltpu.roll(both[c * 8 : c * 8 + 8], SHIFTS[c], 1)
        out_ref[pl.ds(pl.multiple_of(g * 32 + j * 8, 8), 8), :] = total


def place():
    gx, yz = lax.axis_index("gx"), lax.axis_index("yz")
    return lax.div(gx, 2), lax.rem(gx, 2), lax.div(yz, 4), lax.rem(yz, 4)


def column(turn, sign):
    y, _, x, _ = place()
    m = lax.rem(turn + 12, 16)
    ox = lax.rem(m, 4)
    oy = lax.rem(ox + lax.div(m, 4), 4)
    return lax.rem(y + sign * oy + 4, 4), lax.rem(x + sign * ox + 4, 4)


def members(turn, sign):
    _, core, _, z = place()
    y, x = column(turn, sign)
    out = []
    for oc in (0, 1):
        gx = y * 2 + lax.rem(core + oc, 2)
        for oz in range(4):
            out.append((gx, x * 4 + lax.rem(z + oz, 4)))
    return out


def exchange_kernel(
    count_ref, index_ref, gas_hbm, speed_hbm, mass_hbm, offset_hbm, cell_hbm,
    speed_out, mass_out, arrived_ref, wanted_ref,
    gas_ref, speed_ref, mass_ref, offset_ref, cell_ref,
    ask_ref, got_ref, smem_ref, table_ref, send_ref, tiles_ref, deposit_ref, lhs_ref, q_ref,
    load_sems, move_sems, tile_sems,
):
    me = lax.axis_index("gx") * 16 + lax.axis_index("yz")
    barrier = pltpu.get_barrier_semaphore()

    def others(turn, sign, act):
        for n, (gx, yz) in enumerate(members(turn, sign)):
            if n:
                act(gx * 16 + yz, (gx, yz))
            else:
                pl.when(turn != HERE)(functools.partial(act, gx * 16 + yz, (gx, yz)))

    def all_others(act):
        def step(turn, carry):
            others(turn, 1, act)
            return carry

        lax.fori_loop(0, COLUMNS, step, 0)

    all_others(lambda d, to: pl.semaphore_signal(barrier, inc=1, device_id=to, device_id_type=MESH))
    loads = [
        pltpu.make_async_copy(src, dst, load_sems.at[n])
        for n, (src, dst) in enumerate(
            (
                (gas_hbm, gas_ref),
                (speed_hbm, speed_ref),
                (mass_hbm, mass_ref),
                (offset_hbm, offset_ref),
                (cell_hbm, cell_ref),
            )
        )
    ]
    for load in loads:
        load.start()
    asked = jnp.concatenate([index_ref[...], jnp.zeros((124, 128), I32)], axis=0).T
    ask_ref[:, 0, :] = asked
    loads[0].wait()
    make_table(gas_ref, table_ref)
    pl.semaphore_wait(barrier, DEVICES - 1)

    def move(src, dst, sem, to, arrival=None):
        return pltpu.make_async_remote_copy(
            src_ref=src,
            dst_ref=dst,
            send_sem=move_sems.at[sem],
            recv_sem=move_sems.at[sem + 1] if arrival is None else arrival,
            device_id=to,
            device_id_type=MESH,
        )

    partner = (lax.axis_index("gx"), lax.rem(lax.axis_index("yz") + 1, 16))
    all_others(lambda d, to: move(ask_ref.at[d], got_ref.at[me], 0, to).start())
    got_ref[me] = ask_ref[me]
    rest = pl.ds(0, DEVICES - 1)
    asks = move(ask_ref.at[rest], got_ref.at[rest], 0, partner)
    asks.wait_recv()
    down = pltpu.make_async_copy(got_ref, smem_ref, load_sems.at[5])
    down.start()
    down.wait()

    def block(ref, d):
        return ref.at[pl.ds(pl.multiple_of(d * 16, 16), 16)]

    def pick(d, dst):
        for k in range(4):
            dst[pl.ds(pl.multiple_of(d * 16 + k * 4, 4), 4), :] = table_ref[smem_ref[d, 0, k]]

    def pick_column(turn):
        others(turn, 1, lambda d, to: pick(d, send_ref))

    def send_column(turn):
        others(
            turn,
            1,
            lambda d, to: move(block(send_ref, d), block(tiles_ref, me), 2, to, tile_sems.at[turn]).start(),
        )

    def pick_step(turn, carry):
        pick_column(turn)
        send_column(turn - 1)
        return carry

    pick_column(0)
    lax.fori_loop(1, COLUMNS, pick_step, 0)
    send_column(COLUMNS - 1)
    pick(me, tiles_ref)

    for load in loads[1:]:
        load.wait()

    def await_tiles(turn):
        def wait(slots):
            every = pl.ds(0, slots)
            move(send_ref.at[every], tiles_ref.at[every], 2, partner, tile_sems.at[turn]).wait_recv()

        pl.when(turn == HERE)(lambda: wait(7 * 16))
        pl.when(turn != HERE)(lambda: wait(8 * 16))

    def groups(turn):
        y, x = column(turn, -1)
        out = []
        for core in (0, 1):
            g = (y * 2 + core) * 8 + x * 2
            out += [g, g + 1]
        return out

    def first(turn):
        for n, g in enumerate(groups(turn)):
            parcels(g, count_ref, tiles_ref, speed_ref, mass_ref, offset_ref, cell_ref, speed_out, mass_out, lhs_ref.at[n], q_ref.at[n])

    def second(turn):
        for n, g in enumerate(groups(turn)):
            deposits(g, lhs_ref.at[n], q_ref.at[n], deposit_ref)

    def give(turn):
        others(turn, -1, lambda d, to: move(block(deposit_ref, d), block(arrived_ref, me), 3, to).start())

    def step(turn, carry):
        await_tiles(turn)
        second(turn - 1)
        first(turn)
        pl.when(turn > 1)(lambda: give(turn - 2))
        return carry

    await_tiles(0)
    first(0)
    lax.fori_loop(1, COLUMNS, step, 0)
    give(COLUMNS - 2)
    second(COLUMNS - 1)
    wanted_ref[...] = got_ref[:, 0, :].T[:8]
    arrived_ref[pl.ds(pl.multiple_of(me * 16, 16), 16), :] = deposit_ref[pl.ds(pl.multiple_of(me * 16, 16), 16), :]
    give(COLUMNS - 1)

    asks.wait_send()
    rest = pl.ds(0, (DEVICES - 1) * 16)
    move(send_ref.at[rest], tiles_ref.at[rest], 2, partner).wait_send()
    gifts = move(deposit_ref.at[rest], arrived_ref.at[rest], 3, partner)
    gifts.wait_send()
    gifts.wait_recv()


def spread(plane_ref, f, x, xs, halos):
    xlo, xhi, ylo, yhi = halos
    value = plane_ref[f, x]
    row = lax.broadcasted_iota(I32, value.shape, 0)
    lane = lax.broadcasted_iota(I32, value.shape, 1)
    ny, nz = value.shape
    below = xlo[f] if x == 0 else plane_ref[f, x - 1]
    above = xhi[f] if x == xs - 1 else plane_ref[f, x + 1]
    total = below + above
    total = total + jnp.where(row == 0, ylo[f, x : x + 1, :], pltpu.roll(value, 1, 0))
    total = total + jnp.where(row == ny - 1, yhi[f, x : x + 1, :], pltpu.roll(value, ny - 1, 0))
    total = total + jnp.where(lane == 0, 0.0, pltpu.roll(value, 1, 1))
    total = total + jnp.where(lane == nz - 1, 0.0, pltpu.roll(value, nz - 1, 1))
    return value + DIFFUSION * (total - 6.0 * value)


def diffuse_kernel(gas_ref, xlo, xhi, ylo, yhi, out_ref):
    xs = gas_ref.shape[1]

    def step(f, carry):
        for x in range(xs):
            out_ref[f, x] = spread(gas_ref, f, x, xs, (xlo, xhi, ylo, yhi))
        return carry

    lax.fori_loop(0, gas_ref.shape[0], step, 0)


def finish_kernel(base_ref, wanted_ref, arrived_ref, out_ref, sum_ref, hit_ref):
    lane = lanes()
    for part in range(4):
        at = None
        for k in range(4):
            row = jnp.broadcast_to(wanted_ref[pl.ds(k, 1), :], (8, 128))
            mine = jnp.take_along_axis(row, part * 32 + lane // 4, axis=1)
            at = mine if at is None else jnp.where(lane % 4 == k, mine, at)
        at = jnp.broadcast_to(at[:1], (512, 128))
        tile = lax.broadcasted_iota(I32, (512, 128), 0)
        hit_ref[:, pl.ds(part * 128, 128)] = jnp.where(at == tile, 1.0, 0.0).astype(BF16)
    for f in range(4):
        value = arrived_ref[pl.ds(f, 512, stride=4), :]
        high = value.astype(BF16)
        rest = (value - high.astype(F32)).astype(BF16)
        both = jnp.concatenate([high, rest], axis=1)
        both = jnp.dot(hit_ref[...], both, preferred_element_type=F32)
        sum_ref[f] = both[:, :128] + both[:, 128:]
    swaps = chunk_swaps()

    def step(n, carry):
        a, yo = n // 2, n % 2
        y0 = pl.multiple_of(yo * 8, 8)
        for h in (0, 1):
            for f in range(4):
                tiles = []
                for z in (0, 1):
                    tiles.append([])
                    for bh in (0, 1):
                        t0 = (a * 4 + yo * 2 + bh) * 32 + (h * 2 + z) * 8
                        tiles[z].append(sum_ref[f, pl.ds(pl.multiple_of(t0, 8), 8), :])
                blocks = tiles_to_grid(tiles, swaps)
                for u in range(4):
                    at = (a * 4 + u, pl.ds(y0, 8), pl.ds(h * 128, 128))
                    add = blocks[u] * (1.0 / CELL_MASS)
                    if f < 3:
                        out_ref[f, *at] = base_ref[f, *at] + add
                    else:
                        out_ref[3, *at] = base_ref[3, *at] - LATENT_HEAT * add
                        out_ref[4, *at] = base_ref[4, *at] + add
        return carry

    lax.fori_loop(0, 8, step, 0)


VMEM = pl.BlockSpec(memory_space=pltpu.VMEM)
SMEM = pl.BlockSpec(memory_space=pltpu.SMEM)
HBM = pl.BlockSpec(memory_space=pltpu.HBM)


def call(kernel, name, out, in_specs, scratch=(), **params):
    return pl.pallas_call(
        kernel,
        name=name,
        out_shape=out,
        in_specs=in_specs,
        out_specs=jax.tree.map(lambda _: VMEM, out),
        scratch_shapes=scratch,
        compiler_params=pltpu.CompilerParams(vmem_limit_bytes=48 * 1024 * 1024, **params),
    )


def array(*shape, dtype=F32):
    return jax.ShapeDtypeStruct(shape, dtype)


def shards(gas_state, parcel_speed, parcel_mass, offsets, cell_base, block_tile, block_count):
    def three(value):
        return value.reshape(DEVICES, 4, 3, 128).transpose(0, 2, 1, 3).reshape(SLOTS * 3, 128)

    def edges(axis, dim):
        count, length = lax.axis_size(axis), gas_state.shape[dim]
        up = [(i, i + 1) for i in range(count - 1)]
        last = lax.slice_in_dim(gas_state, length - 1, length, axis=dim)
        initial = lax.slice_in_dim(gas_state, 0, 1, axis=dim)
        return (
            jnp.squeeze(lax.ppermute(last, axis, up), dim),
            jnp.squeeze(lax.ppermute(initial, axis, [(b, a) for a, b in up]), dim),
        )

    halos = edges("gx", 1) + edges("yz", 2)
    base = call(diffuse_kernel, "diffuse", array(*gas_state.shape), [VMEM] * 5)(gas_state, *halos)
    dma = pltpu.SemaphoreType.DMA
    speed_next, mass_next, arrived, wanted = call(
        exchange_kernel,
        "exchange",
        (array(SLOTS * 3, 128), array(SLOTS, 128), array(SLOTS * 4, 128), array(8, 128, dtype=I32)),
        [SMEM, VMEM] + [HBM] * 5,
        [
            pltpu.VMEM(gas_state.shape, F32),
            pltpu.VMEM((SLOTS * 3, 128), F32),
            pltpu.VMEM((SLOTS, 128), F32),
            pltpu.VMEM((SLOTS * 3, 128), F32),
            pltpu.VMEM((SLOTS * 3, 128), I32),
            pltpu.VMEM((DEVICES, 1, 128), I32),
            pltpu.VMEM((DEVICES, 1, 128), I32),
            pltpu.SMEM((DEVICES, 1, 128), I32),
            pltpu.VMEM((SLOTS, 4, 128), F32),
            pltpu.VMEM((SLOTS * 4, 128), F32),
            pltpu.VMEM((SLOTS * 4, 128), F32),
            pltpu.VMEM((SLOTS * 4, 128), F32),
            pltpu.VMEM((4, 256, 128), F32),
            pltpu.VMEM((4, 8, 128), I32),
            dma((6,)),
            dma((5,)),
            dma((COLUMNS,)),
        ],
        collective_id=0,
        has_side_effects=True,
    )(
        block_count.reshape(DEVICES),
        block_tile.reshape(DEVICES, 4).T,
        gas_state,
        three(parcel_speed),
        parcel_mass.reshape(SLOTS, 128),
        three(offsets),
        three(cell_base),
    )
    gas_next = call(
        finish_kernel,
        "finish",
        array(*gas_state.shape),
        [VMEM] * 3,
        [pltpu.VMEM((4, SLOTS, 128), F32), pltpu.VMEM((SLOTS, SLOTS), BF16)],
    )(base, wanted, arrived)
    speed_next = speed_next.reshape(DEVICES, 3, 4, 128).transpose(0, 2, 1, 3)
    return gas_next, speed_next.reshape(parcel_speed.shape), mass_next.reshape(parcel_mass.shape)


def solution(mesh):
    in_specs = (
        P(None, "gx", "yz", None),
        P("gx", "yz", None, None, None, None),
        P("gx", "yz", None, None, None),
        P("gx", "yz", None, None, None, None),
        P("gx", "yz", None, None, None, None),
        P("gx", "yz", None, None),
        P("gx", "yz", None),
    )
    out_specs = (
        P(None, "gx", "yz", None),
        P("gx", "yz", None, None, None, None),
        P("gx", "yz", None, None, None),
    )
    return jax.shard_map(shards, mesh=mesh, in_specs=in_specs, out_specs=out_specs, check_vma=False)
```

```python
import functools

import jax
import jax.numpy as jnp
from jax import lax
from jax.experimental import pallas as pl
from jax.experimental.pallas import tpu as pltpu
from jax.sharding import PartitionSpec as P

F32 = jnp.float32
BF16 = jnp.bfloat16
I32 = jnp.int32
MESH = pl.DeviceIdType.MESH

DIFFUSION = 0.1
CELL_MASS = 4.0
DRAG_RATE = 0.5
EVAPORATION = 0.3
LATENT_HEAT = 2.0

SHIFTS = (0, 1, 8, 9, 32, 33, 40, 41)

DEVICES = 128
SLOTS = 512
COLUMNS = 16
HERE = 4


def lanes():
    return lax.broadcasted_iota(I32, (8, 128), 1)


def rows():
    return lax.broadcasted_iota(I32, (8, 128), 0)


def chunk_swaps():
    row, lane = rows(), lanes()
    half, chunk, rest = lane // 64, (lane // 8) % 8, lane % 8
    first = half * 64 + ((chunk - row) % 8) * 8 + rest
    second = (chunk - row) % 8
    third = half * 64 + ((chunk + row) % 8) * 8 + rest
    return first, second, third


def transpose_chunks(block, swaps):
    first, second, third = swaps
    block = jnp.take_along_axis(block, first, axis=1)
    block = jnp.take_along_axis(block, second, axis=0)
    return jnp.take_along_axis(block, third, axis=1)


def swap_halves(a, b, axis):
    size = a.shape[axis] // 2
    low = (lanes() < 64) if axis == 1 else (rows() < 4)
    crossed = pltpu.roll(jnp.where(low, b, a), size, axis)
    return jnp.where(low, a, crossed), jnp.where(low, crossed, b)


def grid_to_tiles(blocks, swaps):
    pairs = [swap_halves(blocks[k], blocks[2 + k], 1) for k in (0, 1)]
    out = []
    for z in (0, 1):
        halves = swap_halves(pairs[0][z], pairs[1][z], 0)
        out.append([transpose_chunks(one, swaps) for one in halves])
    return out


def tiles_to_grid(tiles, swaps):
    pairs = []
    for z in (0, 1):
        a, b = (transpose_chunks(one, swaps) for one in tiles[z])
        pairs.append(swap_halves(a, b, 0))
    blocks = [None] * 4
    for k in (0, 1):
        blocks[k], blocks[2 + k] = swap_halves(pairs[0][k], pairs[1][k], 1)
    return blocks


def make_table(gas_ref, table_ref):
    swaps = chunk_swaps()
    flat_ref = table_ref.reshape(SLOTS * 4, 128)

    def step(n, carry):
        a, yo = n // 2, n % 2
        y0 = pl.multiple_of(yo * 8, 8)
        for h in (0, 1):
            for f in range(4):
                blocks = []
                for u in range(4):
                    part = gas_ref[f, a * 4 + u, pl.ds(y0, 8), pl.ds(h * 128, 128)]
                    if f == 3:
                        part = part - gas_ref[4, a * 4 + u, pl.ds(y0, 8), pl.ds(h * 128, 128)]
                    blocks.append(part)
                tiles = grid_to_tiles(blocks, swaps)
                for z in (0, 1):
                    for bh in (0, 1):
                        t0 = (a * 4 + yo * 2 + bh) * 32 + (h * 2 + z) * 8
                        flat_ref[pl.ds(t0 * 4 + f, 8, stride=4), :] = tiles[z][bh]
        return carry

    lax.fori_loop(0, 8, step, 0)


def split_three(ref, g):
    low = rows() < 4
    v0, v1, v2 = (ref[pl.ds(pl.multiple_of(g * 24 + 8 * n, 8), 8), :] for n in range(3))
    middle = pltpu.roll(jnp.where(low, v2, v0), 4, 0)
    return jnp.where(low, v0, v1), middle, jnp.where(low, v1, v2)


def join_three(ref, g, f0, f1, f2):
    low = rows() < 4
    middle = pltpu.roll(f1, 4, 0)
    out = (jnp.where(low, f0, middle), jnp.where(low, f2, f0), jnp.where(low, middle, f2))
    for n in range(3):
        ref[pl.ds(pl.multiple_of(g * 24 + 8 * n, 8), 8), :] = out[n]


def parcels(g, count_ref, tiles_ref, speed_ref, mass_ref, offset_ref, cell_ref, speed_out, mass_out, lhs_ref, q_ref):
    low = rows() < 4
    cx, cy, cz = split_three(cell_ref, g)
    ox, oy, oz = split_three(offset_ref, g)
    speed = split_three(speed_ref, g)
    mass = mass_ref[pl.ds(pl.multiple_of(g * 8, 8), 8), :]
    q = cx * 32 + cy * 8 + cz
    wx, wy, wz = ((1.0 - o, o) for o in (ox, oy, oz))
    weights = []
    for u in (0, 1):
        for v in (0, 1):
            both = wx[u] * wy[v]
            weights += [both * wz[0], both * wz[1]]
    index = [q + shift for shift in SHIFTS]
    sampled = []
    for f in range(4):
        tile = tiles_ref[pl.ds(g * 32 + f, 8, stride=4), :]
        total = None
        for c in range(8):
            term = jnp.take_along_axis(tile, index[c], axis=1) * weights[c]
            total = term if total is None else total + term
        sampled.append(total)
    log_radius = jnp.log(mass) * (1.0 / 3.0)
    inverse_radius = jnp.exp(-log_radius)
    drag = DRAG_RATE * inverse_radius * inverse_radius
    live = (rows() % 4) < jnp.where(low, count_ref[2 * g], count_ref[2 * g + 1])
    scale = 1.0 / (1.0 + drag)
    gap = sampled[3]
    softplus = jnp.maximum(gap, 0.0) + jnp.log(1.0 + jnp.exp(-jnp.abs(gap)))
    mass_new = mass / (1.0 + EVAPORATION * softplus * inverse_radius)
    mass_new = jnp.where(live, mass_new, mass)
    vapour = mass - mass_new
    speed_new, source = [], []
    for f in range(3):
        moved = jnp.where(live, (speed[f] + drag * sampled[f]) * scale, speed[f])
        speed_new.append(moved)
        source.append(mass * (speed[f] - moved) + vapour * moved)
    source.append(vapour)
    join_three(speed_out, g, *speed_new)
    mass_out[pl.ds(pl.multiple_of(g * 8, 8), 8), :] = mass_new
    for f in range(4):
        value = jnp.where(live, source[f], 0.0)
        for c in range(8):
            lhs_ref[pl.ds(c * 32 + f, 8, stride=4), :] = value * weights[c]
    q_ref[...] = q


def deposits(g, lhs_ref, q_ref, out_ref):
    entry = lax.broadcasted_iota(I32, (128, 128), 0)
    first = lax.broadcasted_iota(I32, (64, 128), 0) % 8 < 4
    keep = jnp.where(first, 1.0, 0.0).astype(BF16)
    drop = jnp.where(first, 0.0, 1.0).astype(BF16)
    for j in range(4):
        left = jnp.concatenate([lhs_ref[pl.ds(c * 32 + j * 8, 8), :] for c in range(8)], axis=0)
        high = left.astype(BF16)
        rest = (left - high.astype(F32)).astype(BF16)
        left = jnp.concatenate(
            [
                jnp.concatenate([high * keep, high * drop], axis=1),
                jnp.concatenate([rest * keep, rest * drop], axis=1),
            ],
            axis=0,
        )
        hits = []
        for k in (0, 1):
            at = jnp.broadcast_to(q_ref[pl.ds(2 * j + k, 1), :], (128, 128))
            hits.append(jnp.where(at == entry, 1.0, 0.0).astype(BF16))
        right = jnp.concatenate(hits, axis=1)
        both = lax.dot_general(left, right, (((1,), (1,)), ((), ())), preferred_element_type=F32)
        both = both[:64] + both[64:]
        total = both[:8]
        for c in range(1, 8):
            total = total + pltpu.roll(both[c * 8 : c * 8 + 8], SHIFTS[c], 1)
        out_ref[pl.ds(pl.multiple_of(g * 32 + j * 8, 8), 8), :] = total


def place():
    gx, yz = lax.axis_index("gx"), lax.axis_index("yz")
    return lax.div(gx, 2), lax.rem(gx, 2), lax.div(yz, 4), lax.rem(yz, 4)


def column(turn, sign):
    y, _, x, _ = place()
    m = lax.rem(turn + 12, 16)
    ox = lax.rem(m, 4)
    oy = lax.rem(ox + lax.div(m, 4), 4)
    return lax.rem(y + sign * oy + 4, 4), lax.rem(x + sign * ox + 4, 4)


def members(turn, sign):
    _, core, _, z = place()
    y, x = column(turn, sign)
    out = []
    for oc in (0, 1):
        gx = y * 2 + lax.rem(core + oc, 2)
        for oz in range(4):
            out.append((gx, x * 4 + lax.rem(z + oz, 4)))
    return out


def exchange_kernel(
    count_hbm, index_hbm, gas_hbm, speed_hbm, mass_hbm, offset_hbm, cell_hbm,
    speed_out, mass_out, arrived_ref, wanted_ref, base_ref,
    gas_ref, speed_ref, mass_ref, offset_ref, cell_ref, count_ref, index_ref,
    ask_ref, got_ref, smem_ref, table_ref, send_ref, tiles_ref, deposit_ref, lhs_ref, q_ref, edge_ref, halo_ref,
    load_sems, move_sems, tile_sems, edge_sems, halo_sems,
):
    gx, yz = lax.axis_index("gx"), lax.axis_index("yz")
    me = gx * 16 + yz
    barrier = pltpu.get_barrier_semaphore()

    def others(turn, sign, act):
        for n, to in enumerate(members(turn, sign)):
            if n:
                act(to[0] * 16 + to[1], to)
            else:
                pl.when(turn != HERE)(functools.partial(act, to[0] * 16 + to[1], to))

    def all_others(act):
        def step(turn, carry):
            others(turn, 1, act)
            return carry

        lax.fori_loop(0, COLUMNS, step, 0)

    loads = [
        pltpu.make_async_copy(src, dst, load_sems.at[n])
        for n, (src, dst) in enumerate(
            (
                (index_hbm, index_ref),
                (gas_hbm, gas_ref),
                (speed_hbm, speed_ref),
                (mass_hbm, mass_ref),
                (offset_hbm, offset_ref),
                (cell_hbm, cell_ref),
                (count_hbm, count_ref),
            )
        )
    ]
    for load in loads:
        load.start()
    all_others(lambda d, to: pl.semaphore_signal(barrier, inc=1, device_id=to, device_id_type=MESH))
    loads[0].wait()
    asked = jnp.concatenate([index_ref[...], jnp.zeros((124, 128), I32)], axis=0).T
    ask_ref[:, 0, :] = asked
    loads[1].wait()
    make_table(gas_ref, table_ref)
    make_edges(gas_ref, edge_ref)
    pl.semaphore_wait(barrier, DEVICES - 1)

    def move(src, dst, sem, to, arrival=None):
        return pltpu.make_async_remote_copy(
            src_ref=src,
            dst_ref=dst,
            send_sem=move_sems.at[sem],
            recv_sem=move_sems.at[sem + 1] if arrival is None else arrival,
            device_id=to,
            device_id_type=MESH,
        )

    partner = (gx, lax.rem(yz + 1, 16))
    all_others(lambda d, to: move(ask_ref.at[d], got_ref.at[me], 0, to).start())
    got_ref[me] = ask_ref[me]

    halos = []
    for n, (here, there, to) in enumerate(
        (
            (gx < 7, gx > 0, (gx + 1, yz)),
            (gx > 0, gx < 7, (gx - 1, yz)),
            (yz < 15, yz > 0, (gx, yz + 1)),
            (yz > 0, yz < 15, (gx, yz - 1)),
        )
    ):
        halo = pltpu.make_async_remote_copy(
            src_ref=edge_ref.at[n],
            dst_ref=halo_ref.at[n],
            send_sem=edge_sems.at[n],
            recv_sem=halo_sems.at[n],
            device_id=to,
            device_id_type=MESH,
        )
        halos.append((here, there, halo))

    def start_halos():
        for n, (here, there, halo) in enumerate(halos):
            pl.when(here)(halo.start)

            @pl.when(jnp.logical_not(there))
            def _(n=n):
                halo_ref[n] = jnp.zeros(halo_ref.shape[1:], F32)

    rest = pl.ds(0, DEVICES - 1)
    asks = move(ask_ref.at[rest], got_ref.at[rest], 0, partner)
    asks.wait_recv()
    wanted_ref[...] = got_ref[:, 0, :].T[:8]
    start_halos()
    down = pltpu.make_async_copy(wanted_ref, smem_ref, load_sems.at[7])
    down.start()
    down.wait()

    def block(ref, d):
        return ref.at[pl.ds(pl.multiple_of(d * 16, 16), 16)]

    def pick(d, dst):
        for k in range(4):
            dst[pl.ds(pl.multiple_of(d * 16 + k * 4, 4), 4), :] = table_ref[smem_ref[k, d]]

    def pick_column(turn):
        others(turn, 1, lambda d, to: pick(d, send_ref))

    def send_column(turn):
        others(
            turn,
            1,
            lambda d, to: move(block(send_ref, d), block(tiles_ref, me), 2, to, tile_sems.at[turn]).start(),
        )

    def pick_step(turn, carry):
        pick_column(turn)
        send_column(turn - 1)
        return carry

    pick_column(0)
    lax.fori_loop(1, COLUMNS, pick_step, 0)
    send_column(COLUMNS - 1)
    pick(me, tiles_ref)

    for load in loads[2:]:
        load.wait()
    for here, there, halo in halos:
        pl.when(there)(halo.wait_recv)
    diffuse(gas_ref, halo_ref, base_ref)

    def await_tiles(turn):
        def wait(slots):
            every = pl.ds(0, slots)
            move(send_ref.at[every], tiles_ref.at[every], 2, partner, tile_sems.at[turn]).wait_recv()

        pl.when(turn == HERE)(lambda: wait(7 * 16))
        pl.when(turn != HERE)(lambda: wait(8 * 16))

    def groups(turn):
        y, x = column(turn, -1)
        out = []
        for core in (0, 1):
            g = (y * 2 + core) * 8 + x * 2
            out += [g, g + 1]
        return out

    def first(turn):
        for n, g in enumerate(groups(turn)):
            parcels(g, count_ref, tiles_ref, speed_ref, mass_ref, offset_ref, cell_ref, speed_out, mass_out, lhs_ref.at[n], q_ref.at[n])

    def second(turn):
        for n, g in enumerate(groups(turn)):
            deposits(g, lhs_ref.at[n], q_ref.at[n], deposit_ref)

    def give(turn):
        others(turn, -1, lambda d, to: move(block(deposit_ref, d), block(arrived_ref, me), 3, to).start())

    def step(turn, carry):
        await_tiles(turn)
        second(turn - 1)
        first(turn)
        pl.when(turn > 1)(lambda: give(turn - 2))
        return carry

    await_tiles(0)
    first(0)
    lax.fori_loop(1, COLUMNS, step, 0)
    give(COLUMNS - 2)
    second(COLUMNS - 1)
    mine = pl.ds(pl.multiple_of(me * 16, 16), 16)
    arrived_ref[mine, :] = deposit_ref[mine, :]
    give(COLUMNS - 1)

    asks.wait_send()
    for here, there, halo in halos:
        pl.when(here)(halo.wait_send)
    rest = pl.ds(0, (DEVICES - 1) * 16)
    move(send_ref.at[rest], tiles_ref.at[rest], 2, partner).wait_send()
    gifts = move(deposit_ref.at[rest], arrived_ref.at[rest], 3, partner)
    gifts.wait_send()
    gifts.wait_recv()


def make_edges(gas_ref, edge_ref):
    def step(f, carry):
        edge_ref[0, f] = gas_ref[f, 15]
        edge_ref[1, f] = gas_ref[f, 0]
        for x in range(16):
            edge_ref[2, f, x : x + 1, :] = gas_ref[f, x, 15:16, :]
            edge_ref[3, f, x : x + 1, :] = gas_ref[f, x, 0:1, :]
        return carry

    lax.fori_loop(0, 5, step, 0)


def spread(plane_ref, f, x, xs, halos):
    xlo, xhi, ylo, yhi = halos
    value = plane_ref[f, x]
    row = lax.broadcasted_iota(I32, value.shape, 0)
    lane = lax.broadcasted_iota(I32, value.shape, 1)
    ny, nz = value.shape
    below = xlo[f] if x == 0 else plane_ref[f, x - 1]
    above = xhi[f] if x == xs - 1 else plane_ref[f, x + 1]
    total = below + above
    total = total + jnp.where(row == 0, ylo[f, x : x + 1, :], pltpu.roll(value, 1, 0))
    total = total + jnp.where(row == ny - 1, yhi[f, x : x + 1, :], pltpu.roll(value, ny - 1, 0))
    total = total + jnp.where(lane == 0, 0.0, pltpu.roll(value, 1, 1))
    total = total + jnp.where(lane == nz - 1, 0.0, pltpu.roll(value, nz - 1, 1))
    return value + DIFFUSION * (total - 6.0 * value)


def diffuse(gas_ref, halo_ref, out_ref):
    xs = gas_ref.shape[1]

    def step(f, carry):
        for x in range(xs):
            out_ref[f, x] = spread(gas_ref, f, x, xs, [halo_ref.at[n] for n in range(4)])
        return carry

    lax.fori_loop(0, gas_ref.shape[0], step, 0)


def finish_kernel(base_ref, wanted_ref, arrived_ref, speed_ref, mass_ref, out_hbm, speed_hbm, mass_hbm, out_ref, sum_ref, hit_ref, sems):
    stores = [
        pltpu.make_async_copy(speed_ref, speed_hbm, sems.at[0]),
        pltpu.make_async_copy(mass_ref, mass_hbm, sems.at[1]),
    ]
    for store in stores:
        store.start()
    lane = lanes()
    for part in range(4):
        at = None
        for k in range(4):
            row = jnp.broadcast_to(wanted_ref[pl.ds(k, 1), :], (8, 128))
            mine = jnp.take_along_axis(row, part * 32 + lane // 4, axis=1)
            at = mine if at is None else jnp.where(lane % 4 == k, mine, at)
        at = jnp.broadcast_to(at[:1], (512, 128))
        tile = lax.broadcasted_iota(I32, (512, 128), 0)
        hit_ref[:, pl.ds(part * 128, 128)] = jnp.where(at == tile, 1.0, 0.0).astype(BF16)
    for f in range(4):
        value = arrived_ref[pl.ds(f, 512, stride=4), :]
        high = value.astype(BF16)
        rest = (value - high.astype(F32)).astype(BF16)
        both = jnp.concatenate([high, rest], axis=1)
        both = jnp.dot(hit_ref[...], both, preferred_element_type=F32)
        sum_ref[f] = both[:, :128] + both[:, 128:]
    swaps = chunk_swaps()

    def step(n, carry):
        a, yo = n // 2, n % 2
        y0 = pl.multiple_of(yo * 8, 8)
        for h in (0, 1):
            for f in range(4):
                tiles = []
                for z in (0, 1):
                    tiles.append([])
                    for bh in (0, 1):
                        t0 = (a * 4 + yo * 2 + bh) * 32 + (h * 2 + z) * 8
                        tiles[z].append(sum_ref[f, pl.ds(pl.multiple_of(t0, 8), 8), :])
                blocks = tiles_to_grid(tiles, swaps)
                for u in range(4):
                    at = (a * 4 + u, pl.ds(y0, 8), pl.ds(h * 128, 128))
                    add = blocks[u] * (1.0 / CELL_MASS)
                    if f < 3:
                        out_ref[f, *at] = base_ref[f, *at] + add
                    else:
                        out_ref[3, *at] = base_ref[3, *at] - LATENT_HEAT * add
                        out_ref[4, *at] = base_ref[4, *at] + add
        return carry

    for a in range(4):
        lax.fori_loop(2 * a, 2 * a + 2, step, 0)
        planes = pl.ds(4 * a, 4)
        store = pltpu.make_async_copy(out_ref.at[:, planes], out_hbm.at[:, planes], sems.at[2 + a])
        store.start()
        stores.append(store)
    for store in stores:
        store.wait()


VMEM = pl.BlockSpec(memory_space=pltpu.VMEM)
SMEM = pl.BlockSpec(memory_space=pltpu.SMEM)
HBM = pl.BlockSpec(memory_space=pltpu.HBM)


def call(kernel, name, out, in_specs, out_specs, scratch=(), limit=48, **params):
    return pl.pallas_call(
        kernel,
        name=name,
        out_shape=out,
        in_specs=in_specs,
        out_specs=out_specs,
        scratch_shapes=scratch,
        compiler_params=pltpu.CompilerParams(vmem_limit_bytes=limit * 1024 * 1024, **params),
    )


def array(*shape, dtype=F32):
    return jax.ShapeDtypeStruct(shape, dtype)


def shards(gas_state, parcel_speed, parcel_mass, offsets, cell_base, block_tile, block_count):
    def three(value):
        return value.reshape(DEVICES, 4, 3, 128).transpose(0, 2, 1, 3).reshape(SLOTS * 3, 128)

    def hbm(value):
        return pltpu.with_memory_space_constraint(value, pltpu.HBM)

    dma = pltpu.SemaphoreType.DMA
    parcel_outs = (array(SLOTS * 3, 128), array(SLOTS, 128))
    grid = array(*gas_state.shape)
    edge = (4, 5, 16, 256)
    speed_next, mass_next, arrived, wanted, base = call(
        exchange_kernel,
        "exchange",
        parcel_outs + (array(SLOTS * 4, 128), array(8, 128, dtype=I32), grid),
        [HBM] * 7,
        (VMEM,) * 5,
        [
            pltpu.VMEM(gas_state.shape, F32),
            pltpu.VMEM((SLOTS * 3, 128), F32),
            pltpu.VMEM((SLOTS, 128), F32),
            pltpu.VMEM((SLOTS * 3, 128), F32),
            pltpu.VMEM((SLOTS * 3, 128), I32),
            pltpu.SMEM((DEVICES,), I32),
            pltpu.VMEM((4, DEVICES), I32),
            pltpu.VMEM((DEVICES, 1, 128), I32),
            pltpu.VMEM((DEVICES, 1, 128), I32),
            pltpu.SMEM((8, 128), I32),
            pltpu.VMEM((SLOTS, 4, 128), F32),
            pltpu.VMEM((SLOTS * 4, 128), F32),
            pltpu.VMEM((SLOTS * 4, 128), F32),
            pltpu.VMEM((SLOTS * 4, 128), F32),
            pltpu.VMEM((4, 256, 128), F32),
            pltpu.VMEM((4, 8, 128), I32),
            pltpu.VMEM(edge, F32),
            pltpu.VMEM(edge, F32),
            dma((8,)),
            dma((5,)),
            dma((COLUMNS,)),
            dma((4,)),
            dma((4,)),
        ],
        limit=48,
        collective_id=0,
        has_side_effects=True,
    )(
        hbm(block_count.reshape(DEVICES)),
        hbm(block_tile.reshape(DEVICES, 4).T),
        hbm(gas_state),
        hbm(three(parcel_speed)),
        hbm(parcel_mass.reshape(SLOTS, 128)),
        hbm(three(offsets)),
        hbm(three(cell_base)),
    )
    gas_next, speed_next, mass_next = call(
        finish_kernel,
        "finish",
        (grid,) + parcel_outs,
        [VMEM] * 5,
        (HBM,) * 3,
        [
            pltpu.VMEM(gas_state.shape, F32),
            pltpu.VMEM((4, SLOTS, 128), F32),
            pltpu.VMEM((SLOTS, SLOTS), BF16),
            dma((6,)),
        ],
    )(base, wanted, arrived, speed_next, mass_next)
    speed_next = speed_next.reshape(DEVICES, 3, 4, 128).transpose(0, 2, 1, 3)
    return gas_next, speed_next.reshape(parcel_speed.shape), mass_next.reshape(parcel_mass.shape)


def solution(mesh):
    in_specs = (
        P(None, "gx", "yz", None),
        P("gx", "yz", None, None, None, None),
        P("gx", "yz", None, None, None),
        P("gx", "yz", None, None, None, None),
        P("gx", "yz", None, None, None, None),
        P("gx", "yz", None, None),
        P("gx", "yz", None),
    )
    out_specs = (
        P(None, "gx", "yz", None),
        P("gx", "yz", None, None, None, None),
        P("gx", "yz", None, None, None),
    )
    return jax.shard_map(shards, mesh=mesh, in_specs=in_specs, out_specs=out_specs, check_vma=False)
```

```python
import functools

import jax
import jax.numpy as jnp
from jax import lax
from jax.experimental import pallas as pl
from jax.experimental.pallas import tpu as pltpu
from jax.sharding import PartitionSpec as P

F32 = jnp.float32
BF16 = jnp.bfloat16
I32 = jnp.int32
MESH = pl.DeviceIdType.MESH

DIFFUSION = 0.1
CELL_MASS = 4.0
DRAG_RATE = 0.5
EVAPORATION = 0.3
LATENT_HEAT = 2.0

SHIFTS = (0, 1, 8, 9, 32, 33, 40, 41)

DEVICES = 128
SLOTS = 512
TURNS = 16
HERE = 0


def lanes():
    return lax.broadcasted_iota(I32, (8, 128), 1)


def rows():
    return lax.broadcasted_iota(I32, (8, 128), 0)


def chunk_swaps():
    row, lane = rows(), lanes()
    half, chunk, rest = lane // 64, (lane // 8) % 8, lane % 8
    first = half * 64 + ((chunk - row) % 8) * 8 + rest
    second = (chunk - row) % 8
    third = half * 64 + ((chunk + row) % 8) * 8 + rest
    return first, second, third


def transpose_chunks(block, swaps):
    first, second, third = swaps
    block = jnp.take_along_axis(block, first, axis=1)
    block = jnp.take_along_axis(block, second, axis=0)
    return jnp.take_along_axis(block, third, axis=1)


def swap_halves(a, b, axis):
    size = a.shape[axis] // 2
    low = (lanes() < 64) if axis == 1 else (rows() < 4)
    crossed = pltpu.roll(jnp.where(low, b, a), size, axis)
    return jnp.where(low, a, crossed), jnp.where(low, crossed, b)


def grid_to_tiles(blocks, swaps):
    pairs = [swap_halves(blocks[k], blocks[2 + k], 1) for k in (0, 1)]
    out = []
    for z in (0, 1):
        halves = swap_halves(pairs[0][z], pairs[1][z], 0)
        out.append([transpose_chunks(one, swaps) for one in halves])
    return out


def tiles_to_grid(tiles, swaps):
    pairs = []
    for z in (0, 1):
        a, b = (transpose_chunks(one, swaps) for one in tiles[z])
        pairs.append(swap_halves(a, b, 0))
    blocks = [None] * 4
    for k in (0, 1):
        blocks[k], blocks[2 + k] = swap_halves(pairs[0][k], pairs[1][k], 1)
    return blocks


def make_table(gas_ref, table_ref):
    swaps = chunk_swaps()
    flat_ref = table_ref.reshape(SLOTS * 4, 128)

    def step(n, carry):
        a, yo = n // 2, n % 2
        y0 = pl.multiple_of(yo * 8, 8)
        for h in (0, 1):
            for f in range(4):
                blocks = []
                for u in range(4):
                    part = gas_ref[f, a * 4 + u, pl.ds(y0, 8), pl.ds(h * 128, 128)]
                    if f == 3:
                        part = part - gas_ref[4, a * 4 + u, pl.ds(y0, 8), pl.ds(h * 128, 128)]
                    blocks.append(part)
                tiles = grid_to_tiles(blocks, swaps)
                for z in (0, 1):
                    for bh in (0, 1):
                        t0 = (a * 4 + yo * 2 + bh) * 32 + (h * 2 + z) * 8
                        flat_ref[pl.ds(t0 * 4 + f, 8, stride=4), :] = tiles[z][bh]
        return carry

    lax.fori_loop(0, 8, step, 0)


def split_three(ref, g):
    low = rows() < 4
    v0, v1, v2 = (ref[pl.ds(pl.multiple_of(g * 24 + 8 * n, 8), 8), :] for n in range(3))
    middle = pltpu.roll(jnp.where(low, v2, v0), 4, 0)
    return jnp.where(low, v0, v1), middle, jnp.where(low, v1, v2)


def join_three(ref, g, f0, f1, f2):
    low = rows() < 4
    middle = pltpu.roll(f1, 4, 0)
    out = (jnp.where(low, f0, middle), jnp.where(low, f2, f0), jnp.where(low, middle, f2))
    for n in range(3):
        ref[pl.ds(pl.multiple_of(g * 24 + 8 * n, 8), 8), :] = out[n]


def parcels(g, count_ref, tiles_ref, speed_ref, mass_ref, offset_ref, cell_ref, speed_out, mass_out, lhs_ref, q_ref):
    low = rows() < 4
    cx, cy, cz = split_three(cell_ref, g)
    ox, oy, oz = split_three(offset_ref, g)
    speed = split_three(speed_ref, g)
    mass = mass_ref[pl.ds(pl.multiple_of(g * 8, 8), 8), :]
    q = cx * 32 + cy * 8 + cz
    wx, wy, wz = ((1.0 - o, o) for o in (ox, oy, oz))
    weights = []
    for u in (0, 1):
        for v in (0, 1):
            both = wx[u] * wy[v]
            weights += [both * wz[0], both * wz[1]]
    index = [q + shift for shift in SHIFTS]
    sampled = []
    for f in range(4):
        tile = tiles_ref[pl.ds(g * 32 + f, 8, stride=4), :]
        total = None
        for c in range(8):
            term = jnp.take_along_axis(tile, index[c], axis=1) * weights[c]
            total = term if total is None else total + term
        sampled.append(total)
    log_radius = jnp.log(mass) * (1.0 / 3.0)
    inverse_radius = jnp.exp(-log_radius)
    drag = DRAG_RATE * inverse_radius * inverse_radius
    live = (rows() % 4) < jnp.where(low, count_ref[2 * g], count_ref[2 * g + 1])
    scale = 1.0 / (1.0 + drag)
    gap = sampled[3]
    softplus = jnp.maximum(gap, 0.0) + jnp.log(1.0 + jnp.exp(-jnp.abs(gap)))
    mass_new = mass / (1.0 + EVAPORATION * softplus * inverse_radius)
    mass_new = jnp.where(live, mass_new, mass)
    vapour = mass - mass_new
    speed_new, source = [], []
    for f in range(3):
        moved = jnp.where(live, (speed[f] + drag * sampled[f]) * scale, speed[f])
        speed_new.append(moved)
        source.append(mass * (speed[f] - moved) + vapour * moved)
    source.append(vapour)
    join_three(speed_out, g, *speed_new)
    mass_out[pl.ds(pl.multiple_of(g * 8, 8), 8), :] = mass_new
    for f in range(4):
        value = jnp.where(live, source[f], 0.0)
        for c in range(8):
            lhs_ref[pl.ds(c * 32 + f, 8, stride=4), :] = value * weights[c]
    q_ref[...] = q


def deposits(g, lhs_ref, q_ref, out_ref):
    entry = lax.broadcasted_iota(I32, (128, 128), 0)
    first = lax.broadcasted_iota(I32, (64, 128), 0) % 8 < 4
    keep = jnp.where(first, 1.0, 0.0).astype(BF16)
    drop = jnp.where(first, 0.0, 1.0).astype(BF16)
    for j in range(4):
        left = jnp.concatenate([lhs_ref[pl.ds(c * 32 + j * 8, 8), :] for c in range(8)], axis=0)
        high = left.astype(BF16)
        rest = (left - high.astype(F32)).astype(BF16)
        left = jnp.concatenate(
            [
                jnp.concatenate([high * keep, high * drop], axis=1),
                jnp.concatenate([rest * keep, rest * drop], axis=1),
            ],
            axis=0,
        )
        hits = []
        for k in (0, 1):
            at = jnp.broadcast_to(q_ref[pl.ds(2 * j + k, 1), :], (128, 128))
            hits.append(jnp.where(at == entry, 1.0, 0.0).astype(BF16))
        right = jnp.concatenate(hits, axis=1)
        both = lax.dot_general(left, right, (((1,), (1,)), ((), ())), preferred_element_type=F32)
        both = both[:64] + both[64:]
        total = both[:8]
        for c in range(1, 8):
            total = total + pltpu.roll(both[c * 8 : c * 8 + 8], SHIFTS[c], 1)
        out_ref[pl.ds(pl.multiple_of(g * 32 + j * 8, 8), 8), :] = total


def place():
    gx, yz = lax.axis_index("gx"), lax.axis_index("yz")
    return lax.div(gx, 2), lax.rem(gx, 2), lax.div(yz, 4), lax.rem(yz, 4)


def pairs(turn, sign):
    y, core, x, z = place()
    k, oc, zb = lax.div(turn, 4), lax.rem(lax.div(turn, 2), 2), lax.rem(turn, 2)
    out = []
    for n in (2, 1, 3, 0):
        gx = lax.rem(y + sign * lax.rem(k + n, 4) + 4, 4) * 2 + lax.rem(core + oc, 2)
        out.append((gx, lax.rem(x + sign * n + 4, 4) * 4 + lax.rem(lax.div(z, 2) + zb + n, 2) * 2))
    return out


def members(turn, sign):
    _, _, _, z = place()
    mine = lax.rem(z, 2)
    out = []
    for gx, yz in pairs(turn, sign):
        out += [(gx, yz + mine), (gx, yz + 1 - mine)]
    return out


def exchange_kernel(
    count_hbm, index_hbm, gas_hbm, speed_hbm, mass_hbm, offset_hbm, cell_hbm,
    speed_out, mass_out, arrived_ref, wanted_ref, base_ref,
    gas_ref, speed_ref, mass_ref, offset_ref, cell_ref, count_ref, index_ref,
    ask_ref, got_ref, smem_ref, table_ref, send_ref, tiles_ref, deposit_ref, lhs_ref, q_ref, edge_ref, halo_ref,
    load_sems, move_sems, ask_sems, down_sems, tile_sems, edge_sems, halo_sems,
):
    gx, yz = lax.axis_index("gx"), lax.axis_index("yz")
    me = gx * 16 + yz
    barrier = pltpu.get_barrier_semaphore()

    def others(turn, sign, act):
        for n, to in enumerate(members(turn, sign)):
            if n != 6:
                act(to[0] * 16 + to[1], to)
            else:
                pl.when(turn != HERE)(functools.partial(act, to[0] * 16 + to[1], to))

    def each_turn(act):
        def step(turn, carry):
            act(turn)
            return carry

        lax.fori_loop(0, TURNS, step, 0)

    loads = [
        pltpu.make_async_copy(src, dst, load_sems.at[n])
        for n, (src, dst) in enumerate(
            (
                (index_hbm, index_ref),
                (gas_hbm, gas_ref),
                (speed_hbm, speed_ref),
                (mass_hbm, mass_ref),
                (offset_hbm, offset_ref),
                (cell_hbm, cell_ref),
                (count_hbm, count_ref),
            )
        )
    ]
    for load in loads:
        load.start()
    def greet(d, to):
        pl.semaphore_signal(barrier, inc=1, device_id=to, device_id_type=MESH)

    each_turn(lambda turn: others(turn, 1, greet))
    loads[0].wait()
    asked = jnp.concatenate([index_ref[...], jnp.zeros((124, 128), I32)], axis=0).T
    ask_ref[:, 0, :] = asked
    loads[1].wait()
    make_table(gas_ref, table_ref)
    make_edges(gas_ref, edge_ref)
    pl.semaphore_wait(barrier, DEVICES - 1)

    def move(src, dst, sem, to, arrival=None):
        return pltpu.make_async_remote_copy(
            src_ref=src,
            dst_ref=dst,
            send_sem=move_sems.at[sem],
            recv_sem=move_sems.at[sem + 1] if arrival is None else arrival,
            device_id=to,
            device_id_type=MESH,
        )

    partner = (gx, lax.rem(yz + 1, 16))

    def ask(turn):
        others(turn, 1, lambda d, to: move(ask_ref.at[d], got_ref.at[me], 0, to, ask_sems.at[turn]).start())

    each_turn(ask)
    got_ref[me] = ask_ref[me]

    halos = []
    for n, (here, there, to) in enumerate(
        (
            (gx < 7, gx > 0, (gx + 1, yz)),
            (gx > 0, gx < 7, (gx - 1, yz)),
            (yz < 15, yz > 0, (gx, yz + 1)),
            (yz > 0, yz < 15, (gx, yz - 1)),
        )
    ):
        halo = pltpu.make_async_remote_copy(
            src_ref=edge_ref.at[n],
            dst_ref=halo_ref.at[n],
            send_sem=edge_sems.at[n],
            recv_sem=halo_sems.at[n],
            device_id=to,
            device_id_type=MESH,
        )
        halos.append((here, there, halo))

    def start_halos():
        for n, (here, there, halo) in enumerate(halos):
            pl.when(here)(halo.start)

            @pl.when(jnp.logical_not(there))
            def _(n=n):
                halo_ref[n] = jnp.zeros(halo_ref.shape[1:], F32)

    start_halos()

    def await_turn(turn, sem, src, dst, per_device):
        def wait(devices):
            every = pl.ds(0, devices * per_device)
            move(src.at[every], dst.at[every], sem[0], partner, sem[1].at[turn]).wait_recv()

        pl.when(turn == HERE)(lambda: wait(7))
        pl.when(turn != HERE)(lambda: wait(8))

    def start_down(turn):
        await_turn(turn, (0, ask_sems), ask_ref, got_ref, 1)
        for x, z in pairs(turn, -1):
            part = pl.ds(x * 16 + z, 2)
            pltpu.make_async_copy(got_ref.at[part], smem_ref.at[part], down_sems.at[turn]).start()

    def await_down(turn):
        part = pl.ds(0, 8)
        pltpu.make_async_copy(got_ref.at[part], smem_ref.at[part], down_sems.at[turn]).wait()

    def block(ref, d):
        return ref.at[pl.ds(pl.multiple_of(d * 16, 16), 16)]

    def pick(d, dst):
        for k in range(4):
            dst[pl.ds(pl.multiple_of(d * 16 + k * 4, 4), 4), :] = table_ref[smem_ref[d, 0, k]]

    def pick_turn(turn):
        await_down(turn)
        others(turn, -1, lambda d, to: pick(d, send_ref))

    def send_turn(turn):
        others(
            turn,
            -1,
            lambda d, to: move(block(send_ref, d), block(tiles_ref, me), 2, to, tile_sems.at[turn]).start(),
        )

    def pick_step(turn, carry):
        pl.when(turn < TURNS - 1)(lambda: start_down(turn + 1))
        pick_turn(turn)
        send_turn(turn - 1)
        return carry

    start_down(0)
    start_down(1)
    pick_turn(0)
    pick(me, tiles_ref)
    lax.fori_loop(1, TURNS, pick_step, 0)
    send_turn(TURNS - 1)
    wanted_ref[...] = got_ref[:, 0, :].T[:8]

    for load in loads[2:]:
        load.wait()
    for here, there, halo in halos:
        pl.when(there)(halo.wait_recv)
    diffuse(gas_ref, halo_ref, base_ref)

    def await_tiles(turn):
        await_turn(turn, (2, tile_sems), send_ref, tiles_ref, 16)

    def groups(turn):
        return [x * 8 + lax.div(z, 2) for x, z in pairs(turn, 1)]

    def first(turn):
        for n, g in enumerate(groups(turn)):
            parcels(g, count_ref, tiles_ref, speed_ref, mass_ref, offset_ref, cell_ref, speed_out, mass_out, lhs_ref.at[n], q_ref.at[n])

    def second(turn):
        for n, g in enumerate(groups(turn)):
            deposits(g, lhs_ref.at[n], q_ref.at[n], deposit_ref)

    def give(turn):
        others(turn, 1, lambda d, to: move(block(deposit_ref, d), block(arrived_ref, me), 3, to).start())

    def step(turn, carry):
        await_tiles(turn)
        second(turn - 1)
        first(turn)
        pl.when(turn > 1)(lambda: give(turn - 2))
        return carry

    await_tiles(0)
    first(0)
    lax.fori_loop(1, TURNS, step, 0)
    give(TURNS - 2)
    second(TURNS - 1)
    mine = pl.ds(pl.multiple_of(me * 16, 16), 16)
    arrived_ref[mine, :] = deposit_ref[mine, :]
    give(TURNS - 1)

    rest = pl.ds(0, DEVICES - 1)
    move(ask_ref.at[rest], got_ref.at[rest], 0, partner).wait_send()
    for here, there, halo in halos:
        pl.when(here)(halo.wait_send)
    rest = pl.ds(0, (DEVICES - 1) * 16)
    move(send_ref.at[rest], tiles_ref.at[rest], 2, partner).wait_send()
    gifts = move(deposit_ref.at[rest], arrived_ref.at[rest], 3, partner)
    gifts.wait_send()
    gifts.wait_recv()


def make_edges(gas_ref, edge_ref):
    def step(f, carry):
        edge_ref[0, f] = gas_ref[f, 15]
        edge_ref[1, f] = gas_ref[f, 0]
        for x in range(16):
            edge_ref[2, f, x : x + 1, :] = gas_ref[f, x, 15:16, :]
            edge_ref[3, f, x : x + 1, :] = gas_ref[f, x, 0:1, :]
        return carry

    lax.fori_loop(0, 5, step, 0)


def spread(plane_ref, f, x, xs, halos):
    xlo, xhi, ylo, yhi = halos
    value = plane_ref[f, x]
    row = lax.broadcasted_iota(I32, value.shape, 0)
    lane = lax.broadcasted_iota(I32, value.shape, 1)
    ny, nz = value.shape
    below = xlo[f] if x == 0 else plane_ref[f, x - 1]
    above = xhi[f] if x == xs - 1 else plane_ref[f, x + 1]
    total = below + above
    total = total + jnp.where(row == 0, ylo[f, x : x + 1, :], pltpu.roll(value, 1, 0))
    total = total + jnp.where(row == ny - 1, yhi[f, x : x + 1, :], pltpu.roll(value, ny - 1, 0))
    total = total + jnp.where(lane == 0, 0.0, pltpu.roll(value, 1, 1))
    total = total + jnp.where(lane == nz - 1, 0.0, pltpu.roll(value, nz - 1, 1))
    return value + DIFFUSION * (total - 6.0 * value)


def diffuse(gas_ref, halo_ref, out_ref):
    xs = gas_ref.shape[1]

    def step(f, carry):
        for x in range(xs):
            out_ref[f, x] = spread(gas_ref, f, x, xs, [halo_ref.at[n] for n in range(4)])
        return carry

    lax.fori_loop(0, gas_ref.shape[0], step, 0)


def finish_kernel(base_ref, wanted_ref, arrived_ref, speed_ref, mass_ref, out_hbm, speed_hbm, mass_hbm, out_ref, sum_ref, hit_ref, sems):
    stores = [
        pltpu.make_async_copy(speed_ref, speed_hbm, sems.at[0]),
        pltpu.make_async_copy(mass_ref, mass_hbm, sems.at[1]),
    ]
    for store in stores:
        store.start()
    lane = lanes()
    for part in range(4):
        at = None
        for k in range(4):
            row = jnp.broadcast_to(wanted_ref[pl.ds(k, 1), :], (8, 128))
            mine = jnp.take_along_axis(row, part * 32 + lane // 4, axis=1)
            at = mine if at is None else jnp.where(lane % 4 == k, mine, at)
        at = jnp.broadcast_to(at[:1], (512, 128))
        tile = lax.broadcasted_iota(I32, (512, 128), 0)
        hit_ref[:, pl.ds(part * 128, 128)] = jnp.where(at == tile, 1.0, 0.0).astype(BF16)
    for f in range(4):
        value = arrived_ref[pl.ds(f, 512, stride=4), :]
        high = value.astype(BF16)
        rest = (value - high.astype(F32)).astype(BF16)
        both = jnp.concatenate([high, rest], axis=1)
        both = jnp.dot(hit_ref[...], both, preferred_element_type=F32)
        sum_ref[f] = both[:, :128] + both[:, 128:]
    swaps = chunk_swaps()

    def planes(a):
        for yo in (0, 1):
            for h in (0, 1):
                for f in range(4):
                    tiles = []
                    for z in (0, 1):
                        tiles.append([])
                        for bh in (0, 1):
                            t0 = (a * 4 + yo * 2 + bh) * 32 + (h * 2 + z) * 8
                            tiles[z].append(sum_ref[f, pl.ds(pl.multiple_of(t0, 8), 8), :])
                    blocks = tiles_to_grid(tiles, swaps)
                    for u in range(4):
                        at = (a * 4 + u, pl.ds(yo * 8, 8), pl.ds(h * 128, 128))
                        add = blocks[u] * (1.0 / CELL_MASS)
                        if f < 3:
                            out_ref[f, *at] = base_ref[f, *at] + add
                        else:
                            out_ref[3, *at] = base_ref[3, *at] - LATENT_HEAT * add
                            out_ref[4, *at] = base_ref[4, *at] + add

    def store(a):
        part = pl.ds(4 * a, 4)
        return pltpu.make_async_copy(out_ref.at[:, part], out_hbm.at[:, part], sems.at[2 + a])

    def step(a, carry):
        planes(a)
        store(a).start()
        return carry

    lax.fori_loop(0, 4, step, 0)
    stores += [store(a) for a in range(4)]
    for store in stores:
        store.wait()


VMEM = pl.BlockSpec(memory_space=pltpu.VMEM)
SMEM = pl.BlockSpec(memory_space=pltpu.SMEM)
HBM = pl.BlockSpec(memory_space=pltpu.HBM)


def call(kernel, name, out, in_specs, out_specs, scratch=(), limit=48, **params):
    return pl.pallas_call(
        kernel,
        name=name,
        out_shape=out,
        in_specs=in_specs,
        out_specs=out_specs,
        scratch_shapes=scratch,
        compiler_params=pltpu.CompilerParams(vmem_limit_bytes=limit * 1024 * 1024, **params),
    )


def array(*shape, dtype=F32):
    return jax.ShapeDtypeStruct(shape, dtype)


def shards(gas_state, parcel_speed, parcel_mass, offsets, cell_base, block_tile, block_count):
    def three(value):
        return value.reshape(DEVICES, 4, 3, 128).transpose(0, 2, 1, 3).reshape(SLOTS * 3, 128)

    def hbm(value):
        return pltpu.with_memory_space_constraint(value, pltpu.HBM)

    dma = pltpu.SemaphoreType.DMA
    parcel_outs = (array(SLOTS * 3, 128), array(SLOTS, 128))
    grid = array(*gas_state.shape)
    edge = (4, 5, 16, 256)
    speed_next, mass_next, arrived, wanted, base = call(
        exchange_kernel,
        "exchange",
        parcel_outs + (array(SLOTS * 4, 128), array(8, 128, dtype=I32), grid),
        [HBM] * 7,
        (VMEM,) * 5,
        [
            pltpu.VMEM(gas_state.shape, F32),
            pltpu.VMEM((SLOTS * 3, 128), F32),
            pltpu.VMEM((SLOTS, 128), F32),
            pltpu.VMEM((SLOTS * 3, 128), F32),
            pltpu.VMEM((SLOTS * 3, 128), I32),
            pltpu.SMEM((DEVICES,), I32),
            pltpu.VMEM((4, DEVICES), I32),
            pltpu.VMEM((DEVICES, 1, 128), I32),
            pltpu.VMEM((DEVICES, 1, 128), I32),
            pltpu.SMEM((DEVICES, 1, 128), I32),
            pltpu.VMEM((SLOTS, 4, 128), F32),
            pltpu.VMEM((SLOTS * 4, 128), F32),
            pltpu.VMEM((SLOTS * 4, 128), F32),
            pltpu.VMEM((SLOTS * 4, 128), F32),
            pltpu.VMEM((4, 256, 128), F32),
            pltpu.VMEM((4, 8, 128), I32),
            pltpu.VMEM(edge, F32),
            pltpu.VMEM(edge, F32),
            dma((7,)),
            dma((5,)),
            dma((TURNS,)),
            dma((TURNS,)),
            dma((TURNS,)),
            dma((4,)),
            dma((4,)),
        ],
        limit=48,
        collective_id=0,
        has_side_effects=True,
    )(
        hbm(block_count.reshape(DEVICES)),
        hbm(block_tile.reshape(DEVICES, 4).T),
        hbm(gas_state),
        hbm(three(parcel_speed)),
        hbm(parcel_mass.reshape(SLOTS, 128)),
        hbm(three(offsets)),
        hbm(three(cell_base)),
    )
    gas_next, speed_next, mass_next = call(
        finish_kernel,
        "finish",
        (grid,) + parcel_outs,
        [VMEM] * 5,
        (HBM,) * 3,
        [
            pltpu.VMEM(gas_state.shape, F32),
            pltpu.VMEM((4, SLOTS, 128), F32),
            pltpu.VMEM((SLOTS, SLOTS), BF16),
            dma((6,)),
        ],
    )(base, wanted, arrived, speed_next, mass_next)
    speed_next = speed_next.reshape(DEVICES, 3, 4, 128).transpose(0, 2, 1, 3)
    return gas_next, speed_next.reshape(parcel_speed.shape), mass_next.reshape(parcel_mass.shape)


def solution(mesh):
    in_specs = (
        P(None, "gx", "yz", None),
        P("gx", "yz", None, None, None, None),
        P("gx", "yz", None, None, None),
        P("gx", "yz", None, None, None, None),
        P("gx", "yz", None, None, None, None),
        P("gx", "yz", None, None),
        P("gx", "yz", None),
    )
    out_specs = (
        P(None, "gx", "yz", None),
        P("gx", "yz", None, None, None, None),
        P("gx", "yz", None, None, None),
    )
    return jax.shard_map(shards, mesh=mesh, in_specs=in_specs, out_specs=out_specs, check_vma=False)
```

```python
import functools

import jax
import jax.numpy as jnp
from jax import lax
from jax.experimental import pallas as pl
from jax.experimental.pallas import tpu as pltpu
from jax.sharding import PartitionSpec as P

F32 = jnp.float32
BF16 = jnp.bfloat16
I32 = jnp.int32
MESH = pl.DeviceIdType.MESH

DIFFUSION = 0.1
CELL_MASS = 4.0
DRAG_RATE = 0.5
EVAPORATION = 0.3
LATENT_HEAT = 2.0

SHIFTS = (0, 1, 8, 9, 32, 33, 40, 41)

DEVICES = 128
SLOTS = 512


def turn_list():
    rings = {
        "near": ((1, 0), (3, 0), (0, 1), (0, 3)),
        "side": ((1, 1), (3, 3), (1, 3), (3, 1)),
        "long": ((2, 1), (2, 3), (1, 2), (3, 2)),
    }
    flags = ((1, 1), (0, 1), (1, 0), (0, 0))
    here = [(0, 0, *flag) for flag in flags]
    far = [(2, 2, *flag) for flag in flags]

    def ring(name, core, z):
        return [(y, x, core, z) for y, x in rings[name]]

    def half(core):
        return [(2, 0, core, 0), (0, 2, core, 0), (2, 0, core, 1), (0, 2, core, 1)]

    return (
        here,
        ring("near", 0, 0),
        ring("near", 1, 1),
        ring("side", 0, 0),
        half(0),
        ring("side", 1, 1),
        half(1),
        ring("side", 0, 1),
        ring("side", 1, 0),
        ring("long", 0, 0),
        ring("long", 1, 1),
        ring("long", 0, 1),
        ring("long", 1, 0),
        far,
        ring("near", 0, 1),
        ring("near", 1, 0),
    )


ORDER = turn_list()
TURNS = len(ORDER)
REACH = ((0, 1), (1, 3), (3, 9), (9, 13), (13, 14))
LATE = (14, 16)
HERE, SELF = 0, 6


def lanes():
    return lax.broadcasted_iota(I32, (8, 128), 1)


def rows():
    return lax.broadcasted_iota(I32, (8, 128), 0)


def chunk_swaps():
    row, lane = rows(), lanes()
    half, chunk, rest = lane // 64, (lane // 8) % 8, lane % 8
    first = half * 64 + ((chunk - row) % 8) * 8 + rest
    second = (chunk - row) % 8
    third = half * 64 + ((chunk + row) % 8) * 8 + rest
    return first, second, third


def transpose_chunks(block, swaps):
    first, second, third = swaps
    block = jnp.take_along_axis(block, first, axis=1)
    block = jnp.take_along_axis(block, second, axis=0)
    return jnp.take_along_axis(block, third, axis=1)


def swap_halves(a, b, axis):
    size = a.shape[axis] // 2
    low = (lanes() < 64) if axis == 1 else (rows() < 4)
    crossed = pltpu.roll(jnp.where(low, b, a), size, axis)
    return jnp.where(low, a, crossed), jnp.where(low, crossed, b)


def grid_to_tiles(blocks, swaps):
    pairs = [swap_halves(blocks[k], blocks[2 + k], 1) for k in (0, 1)]
    out = []
    for z in (0, 1):
        halves = swap_halves(pairs[0][z], pairs[1][z], 0)
        out.append([transpose_chunks(one, swaps) for one in halves])
    return out


def tiles_to_grid(tiles, swaps):
    pairs = []
    for z in (0, 1):
        a, b = (transpose_chunks(one, swaps) for one in tiles[z])
        pairs.append(swap_halves(a, b, 0))
    blocks = [None] * 4
    for k in (0, 1):
        blocks[k], blocks[2 + k] = swap_halves(pairs[0][k], pairs[1][k], 1)
    return blocks


def make_table(gas_ref, table_ref, part):
    swaps = chunk_swaps()
    flat_ref = table_ref.reshape(SLOTS * 4, 128)

    def step(n, carry):
        a, yo = n // 2, n % 2
        y0 = pl.multiple_of(yo * 8, 8)
        for h in (0, 1):
            for f in range(4):
                blocks = []
                for u in range(4):
                    part = gas_ref[f, a * 4 + u, pl.ds(y0, 8), pl.ds(h * 128, 128)]
                    if f == 3:
                        part = part - gas_ref[4, a * 4 + u, pl.ds(y0, 8), pl.ds(h * 128, 128)]
                    blocks.append(part)
                tiles = grid_to_tiles(blocks, swaps)
                for z in (0, 1):
                    for bh in (0, 1):
                        t0 = (a * 4 + yo * 2 + bh) * 32 + (h * 2 + z) * 8
                        flat_ref[pl.ds(t0 * 4 + f, 8, stride=4), :] = tiles[z][bh]
        return carry

    lax.fori_loop(2 * part, 2 * part + 2, step, 0)


def split_three(ref, g):
    low = rows() < 4
    v0, v1, v2 = (ref[pl.ds(pl.multiple_of(g * 24 + 8 * n, 8), 8), :] for n in range(3))
    middle = pltpu.roll(jnp.where(low, v2, v0), 4, 0)
    return jnp.where(low, v0, v1), middle, jnp.where(low, v1, v2)


def join_three(ref, g, f0, f1, f2):
    low = rows() < 4
    middle = pltpu.roll(f1, 4, 0)
    out = (jnp.where(low, f0, middle), jnp.where(low, f2, f0), jnp.where(low, middle, f2))
    for n in range(3):
        ref[pl.ds(pl.multiple_of(g * 24 + 8 * n, 8), 8), :] = out[n]


def parcels(g, count_ref, tiles_ref, speed_ref, mass_ref, offset_ref, cell_ref, speed_out, mass_out, lhs_ref, q_ref):
    low = rows() < 4
    cx, cy, cz = split_three(cell_ref, g)
    ox, oy, oz = split_three(offset_ref, g)
    speed = split_three(speed_ref, g)
    mass = mass_ref[pl.ds(pl.multiple_of(g * 8, 8), 8), :]
    q = cx * 32 + cy * 8 + cz
    wx, wy, wz = ((1.0 - o, o) for o in (ox, oy, oz))
    weights = []
    for u in (0, 1):
        for v in (0, 1):
            both = wx[u] * wy[v]
            weights += [both * wz[0], both * wz[1]]
    index = [q + shift for shift in SHIFTS]
    sampled = []
    for f in range(4):
        tile = tiles_ref[pl.ds(g * 32 + f, 8, stride=4), :]
        total = None
        for c in range(8):
            term = jnp.take_along_axis(tile, index[c], axis=1) * weights[c]
            total = term if total is None else total + term
        sampled.append(total)
    log_radius = jnp.log(mass) * (1.0 / 3.0)
    inverse_radius = jnp.exp(-log_radius)
    drag = DRAG_RATE * inverse_radius * inverse_radius
    live = (rows() % 4) < jnp.where(low, count_ref[2 * g], count_ref[2 * g + 1])
    scale = 1.0 / (1.0 + drag)
    gap = sampled[3]
    softplus = jnp.maximum(gap, 0.0) + jnp.log(1.0 + jnp.exp(-jnp.abs(gap)))
    mass_new = mass / (1.0 + EVAPORATION * softplus * inverse_radius)
    mass_new = jnp.where(live, mass_new, mass)
    vapour = mass - mass_new
    speed_new, source = [], []
    for f in range(3):
        moved = jnp.where(live, (speed[f] + drag * sampled[f]) * scale, speed[f])
        speed_new.append(moved)
        source.append(mass * (speed[f] - moved) + vapour * moved)
    source.append(vapour)
    join_three(speed_out, g, *speed_new)
    mass_out[pl.ds(pl.multiple_of(g * 8, 8), 8), :] = mass_new
    for f in range(4):
        value = jnp.where(live, source[f], 0.0)
        for c in range(8):
            lhs_ref[pl.ds(c * 32 + f, 8, stride=4), :] = value * weights[c]
    q_ref[...] = q


def deposits(g, lhs_ref, q_ref, out_ref):
    entry = lax.broadcasted_iota(I32, (128, 128), 0)
    first = lax.broadcasted_iota(I32, (64, 128), 0) % 8 < 4
    keep = jnp.where(first, 1.0, 0.0).astype(BF16)
    drop = jnp.where(first, 0.0, 1.0).astype(BF16)
    for j in range(4):
        left = jnp.concatenate([lhs_ref[pl.ds(c * 32 + j * 8, 8), :] for c in range(8)], axis=0)
        high = left.astype(BF16)
        rest = (left - high.astype(F32)).astype(BF16)
        left = jnp.concatenate(
            [
                jnp.concatenate([high * keep, high * drop], axis=1),
                jnp.concatenate([rest * keep, rest * drop], axis=1),
            ],
            axis=0,
        )
        hits = []
        for k in (0, 1):
            at = jnp.broadcast_to(q_ref[pl.ds(2 * j + k, 1), :], (128, 128))
            hits.append(jnp.where(at == entry, 1.0, 0.0).astype(BF16))
        right = jnp.concatenate(hits, axis=1)
        both = lax.dot_general(left, right, (((1,), (1,)), ((), ())), preferred_element_type=F32)
        both = both[:64] + both[64:]
        total = both[:8]
        for c in range(1, 8):
            total = total + pltpu.roll(both[c * 8 : c * 8 + 8], SHIFTS[c], 1)
        out_ref[pl.ds(pl.multiple_of(g * 32 + j * 8, 8), 8), :] = total


def place():
    gx, yz = lax.axis_index("gx"), lax.axis_index("yz")
    return lax.div(gx, 2), lax.rem(gx, 2), lax.div(yz, 4), lax.rem(yz, 4)


def choose(turn, values):
    if isinstance(turn, int):
        return values[turn]
    bit = 1
    while len(values) > 1:
        odd = lax.rem(lax.div(turn, bit), 2) == 1
        values = [a if isinstance(a, int) and isinstance(b, int) and a == b else jnp.where(odd, b, a) for a, b in zip(values[::2], values[1::2])]
        bit *= 2
    return values[0]


def pairs(turn, sign):
    y, core, x, z = place()
    out = []
    for n in range(4):
        oy, ox, oc, oz = (choose(turn, [one[n][part] for one in ORDER]) for part in range(4))
        gx = lax.rem(y + sign * oy + 4, 4) * 2 + lax.rem(core + oc, 2)
        out.append((gx, lax.rem(x + sign * ox + 4, 4) * 4 + lax.rem(lax.div(z, 2) + oz, 2) * 2))
    return out


def members(turn, sign):
    _, _, _, z = place()
    mine = lax.rem(z, 2)
    out = []
    for gx, yz in pairs(turn, sign):
        out += [(gx, yz + mine), (gx, yz + 1 - mine)]
    return out


def exchange_kernel(
    count_hbm, index_hbm, gas_hbm, speed_hbm, mass_hbm, offset_hbm, cell_hbm,
    speed_out, mass_out, arrived_ref, wanted_ref, base_ref,
    gas_ref, speed_ref, mass_ref, offset_ref, cell_ref, count_ref, index_ref,
    ask_ref, got_ref, smem_ref, table_ref, send_ref, tiles_ref, deposit_ref, lhs_ref, q_ref, edge_ref, halo_ref,
    near_sems, load_sems, move_sems, ask_sems, down_sems, tile_sems, edge_sems, halo_sems,
):
    gx, yz = lax.axis_index("gx"), lax.axis_index("yz")
    me = gx * 16 + yz
    barrier = pltpu.get_barrier_semaphore()

    def others(turn, sign, act):
        for n, to in enumerate(members(turn, sign)):
            one = functools.partial(act, to[0] * 16 + to[1], to)
            if n != SELF:
                one()
            elif isinstance(turn, int):
                if turn != HERE:
                    one()
            else:
                pl.when(turn != HERE)(one)

    loads = [
        pltpu.make_async_copy(src, dst, load_sems.at[n])
        for n, (src, dst) in enumerate(
            (
                (index_hbm, index_ref),
                (gas_hbm, gas_ref),
                (speed_hbm, speed_ref),
                (mass_hbm, mass_ref),
                (offset_hbm, offset_ref),
                (cell_hbm, cell_ref),
                (count_hbm, count_ref),
            )
        )
    ]
    for load in loads:
        load.start()
    y, core, x, z = place()
    beside = [
        (lax.rem(y + step, 4) * 2 + core, lax.rem(x + other, 4) * 4 + z)
        for step, other in ((1, 0), (3, 0), (0, 1), (0, 3))
    ]
    mates = [(y * 2 + lax.rem(core + n // 4, 2), x * 4 + lax.rem(z + n, 4)) for n in range(1, 8)]
    for to in mates + beside:
        pl.semaphore_signal(barrier, inc=1, device_id=to, device_id_type=MESH)
    loads[0].wait()
    asked = jnp.concatenate([index_ref[...], jnp.zeros((124, 128), I32)], axis=0).T
    ask_ref[:, 0, :] = asked
    def move(src, dst, sem, to, arrival=None):
        return pltpu.make_async_remote_copy(
            src_ref=src,
            dst_ref=dst,
            send_sem=move_sems.at[sem],
            recv_sem=move_sems.at[sem + 1] if arrival is None else arrival,
            device_id=to,
            device_id_type=MESH,
        )

    partner = (gx, lax.rem(yz + 1, 16))

    def ask(turn):
        others(turn, 1, lambda d, to: move(ask_ref.at[d], got_ref.at[me], 0, to, ask_sems.at[turn]).start())

    def ask_turns(turns):
        for turn in range(*turns):
            ask(turn)

    got_ref[me] = ask_ref[me]
    pl.semaphore_wait(barrier, len(mates + beside))
    for n, turns in enumerate(REACH):
        if n < 4:
            for to in beside:
                pl.semaphore_signal(near_sems.at[n], inc=1, device_id=to, device_id_type=MESH)
        ask_turns(turns)
        if n == 1:
            ask_turns(LATE)
        if n == 0:
            loads[1].wait()
        if n < 4:
            make_table(gas_ref, table_ref, n)
            pl.semaphore_wait(near_sems.at[n], len(beside))
    make_edges(gas_ref, edge_ref)

    halos = []
    for n, (here, there, to) in enumerate(
        (
            (gx < 7, gx > 0, (gx + 1, yz)),
            (gx > 0, gx < 7, (gx - 1, yz)),
            (yz < 15, yz > 0, (gx, yz + 1)),
            (yz > 0, yz < 15, (gx, yz - 1)),
        )
    ):
        halo = pltpu.make_async_remote_copy(
            src_ref=edge_ref.at[n],
            dst_ref=halo_ref.at[n],
            send_sem=edge_sems.at[n],
            recv_sem=halo_sems.at[n],
            device_id=to,
            device_id_type=MESH,
        )
        halos.append((here, there, halo))

    def start_halos():
        for n, (here, there, halo) in enumerate(halos):
            pl.when(here)(halo.start)

            @pl.when(jnp.logical_not(there))
            def _(n=n):
                halo_ref[n] = jnp.zeros(halo_ref.shape[1:], F32)

    start_halos()

    def await_turn(turn, sem, src, dst, per_device):
        def wait(devices):
            every = pl.ds(0, devices * per_device)
            move(src.at[every], dst.at[every], sem[0], partner, sem[1].at[turn]).wait_recv()

        pl.when(turn == HERE)(lambda: wait(7))
        pl.when(turn != HERE)(lambda: wait(8))

    def start_down(turn):
        await_turn(turn, (0, ask_sems), ask_ref, got_ref, 1)
        for to in pairs(turn, -1):
            part = pl.ds(to[0] * 16 + to[1], 2)
            pltpu.make_async_copy(got_ref.at[part], smem_ref.at[part], down_sems.at[turn]).start()

    def await_down(turn):
        part = pl.ds(0, 8)
        pltpu.make_async_copy(got_ref.at[part], smem_ref.at[part], down_sems.at[turn]).wait()

    def block(ref, d):
        return ref.at[pl.ds(pl.multiple_of(d * 16, 16), 16)]

    def pick(d, dst):
        for k in range(4):
            dst[pl.ds(pl.multiple_of(d * 16 + k * 4, 4), 4), :] = table_ref[smem_ref[d, 0, k]]

    def pick_turn(turn):
        await_down(turn)
        others(turn, -1, lambda d, to: pick(d, send_ref))

    def send_turn(turn):
        others(
            turn,
            -1,
            lambda d, to: move(block(send_ref, d), block(tiles_ref, me), 2, to, tile_sems.at[turn]).start(),
        )

    def pick_step(turn, carry):
        pl.when(turn < TURNS - 1)(lambda: start_down(turn + 1))
        pick_turn(turn)
        send_turn(turn - 1)
        return carry

    start_down(0)
    start_down(1)
    pick_turn(0)
    pick(me, tiles_ref)
    lax.fori_loop(1, TURNS, pick_step, 0)
    send_turn(TURNS - 1)
    wanted_ref[...] = got_ref[:, 0, :].T[:8]

    for load in loads[2:]:
        load.wait()
    for here, there, halo in halos:
        pl.when(there)(halo.wait_recv)
    diffuse(gas_ref, halo_ref, base_ref)

    def await_tiles(turn):
        await_turn(turn, (2, tile_sems), send_ref, tiles_ref, 16)

    def groups(turn):
        return [to[0] * 8 + lax.div(to[1], 2) for to in pairs(turn, 1)]

    def first(turn):
        for n, g in enumerate(groups(turn)):
            parcels(g, count_ref, tiles_ref, speed_ref, mass_ref, offset_ref, cell_ref, speed_out, mass_out, lhs_ref.at[n], q_ref.at[n])

    def second(turn):
        for n, g in enumerate(groups(turn)):
            deposits(g, lhs_ref.at[n], q_ref.at[n], deposit_ref)

    def give(turn):
        others(turn, 1, lambda d, to: move(block(deposit_ref, d), block(arrived_ref, me), 3, to).start())

    def step(turn, carry):
        await_tiles(turn)
        second(turn - 1)
        first(turn)
        pl.when(turn > 1)(lambda: give(turn - 2))
        return carry

    await_tiles(0)
    first(0)
    lax.fori_loop(1, TURNS, step, 0)
    give(TURNS - 2)
    second(TURNS - 1)
    mine = pl.ds(pl.multiple_of(me * 16, 16), 16)
    arrived_ref[mine, :] = deposit_ref[mine, :]
    give(TURNS - 1)

    rest = pl.ds(0, DEVICES - 1)
    move(ask_ref.at[rest], got_ref.at[rest], 0, partner).wait_send()
    for here, there, halo in halos:
        pl.when(here)(halo.wait_send)
    rest = pl.ds(0, (DEVICES - 1) * 16)
    move(send_ref.at[rest], tiles_ref.at[rest], 2, partner).wait_send()
    gifts = move(deposit_ref.at[rest], arrived_ref.at[rest], 3, partner)
    gifts.wait_send()
    gifts.wait_recv()


def make_edges(gas_ref, edge_ref):
    def step(f, carry):
        edge_ref[0, f] = gas_ref[f, 15]
        edge_ref[1, f] = gas_ref[f, 0]
        for x in range(16):
            edge_ref[2, f, x : x + 1, :] = gas_ref[f, x, 15:16, :]
            edge_ref[3, f, x : x + 1, :] = gas_ref[f, x, 0:1, :]
        return carry

    lax.fori_loop(0, 5, step, 0)


def spread(plane_ref, f, x, xs, halos):
    xlo, xhi, ylo, yhi = halos
    value = plane_ref[f, x]
    row = lax.broadcasted_iota(I32, value.shape, 0)
    lane = lax.broadcasted_iota(I32, value.shape, 1)
    ny, nz = value.shape
    below = xlo[f] if x == 0 else plane_ref[f, x - 1]
    above = xhi[f] if x == xs - 1 else plane_ref[f, x + 1]
    total = below + above
    total = total + jnp.where(row == 0, ylo[f, x : x + 1, :], pltpu.roll(value, 1, 0))
    total = total + jnp.where(row == ny - 1, yhi[f, x : x + 1, :], pltpu.roll(value, ny - 1, 0))
    total = total + jnp.where(lane == 0, 0.0, pltpu.roll(value, 1, 1))
    total = total + jnp.where(lane == nz - 1, 0.0, pltpu.roll(value, nz - 1, 1))
    return value + DIFFUSION * (total - 6.0 * value)


def diffuse(gas_ref, halo_ref, out_ref):
    xs = gas_ref.shape[1]

    def step(f, carry):
        for x in range(xs):
            out_ref[f, x] = spread(gas_ref, f, x, xs, [halo_ref.at[n] for n in range(4)])
        return carry

    lax.fori_loop(0, gas_ref.shape[0], step, 0)


def finish_kernel(base_ref, wanted_ref, arrived_ref, speed_ref, mass_ref, out_hbm, speed_hbm, mass_hbm, out_ref, sum_ref, hit_ref, sems):
    stores = [
        pltpu.make_async_copy(speed_ref, speed_hbm, sems.at[0]),
        pltpu.make_async_copy(mass_ref, mass_hbm, sems.at[1]),
    ]
    for store in stores:
        store.start()
    lane = lanes()
    for part in range(4):
        at = None
        for k in range(4):
            row = jnp.broadcast_to(wanted_ref[pl.ds(k, 1), :], (8, 128))
            mine = jnp.take_along_axis(row, part * 32 + lane // 4, axis=1)
            at = mine if at is None else jnp.where(lane % 4 == k, mine, at)
        at = jnp.broadcast_to(at[:1], (512, 128))
        tile = lax.broadcasted_iota(I32, (512, 128), 0)
        hit_ref[:, pl.ds(part * 128, 128)] = jnp.where(at == tile, 1.0, 0.0).astype(BF16)
    for f in range(4):
        value = arrived_ref[pl.ds(f, 512, stride=4), :]
        high = value.astype(BF16)
        rest = (value - high.astype(F32)).astype(BF16)
        both = jnp.concatenate([high, rest], axis=1)
        both = jnp.dot(hit_ref[...], both, preferred_element_type=F32)
        sum_ref[f] = both[:, :128] + both[:, 128:]
    swaps = chunk_swaps()

    def planes(a):
        for yo in (0, 1):
            for h in (0, 1):
                for f in range(4):
                    tiles = []
                    for z in (0, 1):
                        tiles.append([])
                        for bh in (0, 1):
                            t0 = (a * 4 + yo * 2 + bh) * 32 + (h * 2 + z) * 8
                            tiles[z].append(sum_ref[f, pl.ds(pl.multiple_of(t0, 8), 8), :])
                    blocks = tiles_to_grid(tiles, swaps)
                    for u in range(4):
                        at = (a * 4 + u, pl.ds(yo * 8, 8), pl.ds(h * 128, 128))
                        add = blocks[u] * (1.0 / CELL_MASS)
                        if f < 3:
                            out_ref[f, *at] = base_ref[f, *at] + add
                        else:
                            out_ref[3, *at] = base_ref[3, *at] - LATENT_HEAT * add
                            out_ref[4, *at] = base_ref[4, *at] + add

    def store(a):
        part = pl.ds(4 * a, 4)
        return pltpu.make_async_copy(out_ref.at[:, part], out_hbm.at[:, part], sems.at[2 + a])

    def step(a, carry):
        planes(a)
        store(a).start()
        return carry

    lax.fori_loop(0, 4, step, 0)
    stores += [store(a) for a in range(4)]
    for store in stores:
        store.wait()


VMEM = pl.BlockSpec(memory_space=pltpu.VMEM)
SMEM = pl.BlockSpec(memory_space=pltpu.SMEM)
HBM = pl.BlockSpec(memory_space=pltpu.HBM)


def call(kernel, name, out, in_specs, out_specs, scratch=(), limit=48, **params):
    return pl.pallas_call(
        kernel,
        name=name,
        out_shape=out,
        in_specs=in_specs,
        out_specs=out_specs,
        scratch_shapes=scratch,
        compiler_params=pltpu.CompilerParams(vmem_limit_bytes=limit * 1024 * 1024, **params),
    )


def array(*shape, dtype=F32):
    return jax.ShapeDtypeStruct(shape, dtype)


def shards(gas_state, parcel_speed, parcel_mass, offsets, cell_base, block_tile, block_count):
    def three(value):
        return value.reshape(DEVICES, 4, 3, 128).transpose(0, 2, 1, 3).reshape(SLOTS * 3, 128)

    def hbm(value):
        return pltpu.with_memory_space_constraint(value, pltpu.HBM)

    dma = pltpu.SemaphoreType.DMA
    parcel_outs = (array(SLOTS * 3, 128), array(SLOTS, 128))
    grid = array(*gas_state.shape)
    edge = (4, 5, 16, 256)
    speed_next, mass_next, arrived, wanted, base = call(
        exchange_kernel,
        "exchange",
        parcel_outs + (array(SLOTS * 4, 128), array(8, 128, dtype=I32), grid),
        [HBM] * 7,
        (VMEM,) * 5,
        [
            pltpu.VMEM(gas_state.shape, F32),
            pltpu.VMEM((SLOTS * 3, 128), F32),
            pltpu.VMEM((SLOTS, 128), F32),
            pltpu.VMEM((SLOTS * 3, 128), F32),
            pltpu.VMEM((SLOTS * 3, 128), I32),
            pltpu.SMEM((DEVICES,), I32),
            pltpu.VMEM((4, DEVICES), I32),
            pltpu.VMEM((DEVICES, 1, 128), I32),
            pltpu.VMEM((DEVICES, 1, 128), I32),
            pltpu.SMEM((DEVICES, 1, 128), I32),
            pltpu.VMEM((SLOTS, 4, 128), F32),
            pltpu.VMEM((SLOTS * 4, 128), F32),
            pltpu.VMEM((SLOTS * 4, 128), F32),
            pltpu.VMEM((SLOTS * 4, 128), F32),
            pltpu.VMEM((4, 256, 128), F32),
            pltpu.VMEM((4, 8, 128), I32),
            pltpu.VMEM(edge, F32),
            pltpu.VMEM(edge, F32),
            pltpu.SemaphoreType.REGULAR((4,)),
            dma((7,)),
            dma((5,)),
            dma((TURNS,)),
            dma((TURNS,)),
            dma((TURNS,)),
            dma((4,)),
            dma((4,)),
        ],
        limit=48,
        collective_id=0,
        has_side_effects=True,
    )(
        hbm(block_count.reshape(DEVICES)),
        hbm(block_tile.reshape(DEVICES, 4).T),
        hbm(gas_state),
        hbm(three(parcel_speed)),
        hbm(parcel_mass.reshape(SLOTS, 128)),
        hbm(three(offsets)),
        hbm(three(cell_base)),
    )
    gas_next, speed_next, mass_next = call(
        finish_kernel,
        "finish",
        (grid,) + parcel_outs,
        [VMEM] * 5,
        (HBM,) * 3,
        [
            pltpu.VMEM(gas_state.shape, F32),
            pltpu.VMEM((4, SLOTS, 128), F32),
            pltpu.VMEM((SLOTS, SLOTS), BF16),
            dma((6,)),
        ],
    )(base, wanted, arrived, speed_next, mass_next)
    speed_next = speed_next.reshape(DEVICES, 3, 4, 128).transpose(0, 2, 1, 3)
    return gas_next, speed_next.reshape(parcel_speed.shape), mass_next.reshape(parcel_mass.shape)


def solution(mesh):
    in_specs = (
        P(None, "gx", "yz", None),
        P("gx", "yz", None, None, None, None),
        P("gx", "yz", None, None, None),
        P("gx", "yz", None, None, None, None),
        P("gx", "yz", None, None, None, None),
        P("gx", "yz", None, None),
        P("gx", "yz", None),
    )
    out_specs = (
        P(None, "gx", "yz", None),
        P("gx", "yz", None, None, None, None),
        P("gx", "yz", None, None, None),
    )
    return jax.shard_map(shards, mesh=mesh, in_specs=in_specs, out_specs=out_specs, check_vma=False)
```

```python
import functools

import jax
import jax.numpy as jnp
from jax import lax
from jax.experimental import pallas as pl
from jax.experimental.pallas import tpu as pltpu
from jax.sharding import PartitionSpec as P

F32 = jnp.float32
BF16 = jnp.bfloat16
I32 = jnp.int32
MESH = pl.DeviceIdType.MESH

DIFFUSION = 0.1
CELL_MASS = 4.0
DRAG_RATE = 0.5
EVAPORATION = 0.3
LATENT_HEAT = 2.0

SHIFTS = (0, 1, 8, 9, 32, 33, 40, 41)

DEVICES = 128
SLOTS = 512


def turn_list():
    rings = {
        "near": ((1, 0), (3, 0), (0, 1), (0, 3)),
        "side": ((1, 1), (3, 3), (1, 3), (3, 1)),
        "long": ((2, 1), (2, 3), (1, 2), (3, 2)),
    }
    flags = ((1, 1), (0, 1), (1, 0), (0, 0))
    here = [(0, 0, *flag) for flag in flags]
    far = [(2, 2, *flag) for flag in flags]

    def ring(name, core, z):
        return [(y, x, core, z) for y, x in rings[name]]

    def half(core):
        return [(2, 0, core, 0), (0, 2, core, 0), (2, 0, core, 1), (0, 2, core, 1)]

    return (
        here,
        ring("near", 0, 0),
        ring("near", 1, 1),
        ring("side", 0, 0),
        half(0),
        ring("side", 1, 1),
        half(1),
        ring("side", 0, 1),
        ring("side", 1, 0),
        ring("long", 0, 0),
        ring("long", 1, 1),
        ring("long", 0, 1),
        ring("long", 1, 0),
        far,
        ring("near", 0, 1),
        ring("near", 1, 0),
    )


ORDER = turn_list()
TURNS = len(ORDER)
REACH = ((0, 1), (1, 3), (3, 9), (9, 13), (13, 14))
LATE = (14, 16)
HERE, SELF = 0, 6


def lanes():
    return lax.broadcasted_iota(I32, (8, 128), 1)


def rows():
    return lax.broadcasted_iota(I32, (8, 128), 0)


def chunk_swaps():
    row, lane = rows(), lanes()
    half, chunk, rest = lane // 64, (lane // 8) % 8, lane % 8
    first = half * 64 + ((chunk - row) % 8) * 8 + rest
    second = (chunk - row) % 8
    third = half * 64 + ((chunk + row) % 8) * 8 + rest
    return first, second, third


def transpose_chunks(block, swaps):
    first, second, third = swaps
    block = jnp.take_along_axis(block, first, axis=1)
    block = jnp.take_along_axis(block, second, axis=0)
    return jnp.take_along_axis(block, third, axis=1)


def swap_halves(a, b, axis):
    size = a.shape[axis] // 2
    low = (lanes() < 64) if axis == 1 else (rows() < 4)
    crossed = pltpu.roll(jnp.where(low, b, a), size, axis)
    return jnp.where(low, a, crossed), jnp.where(low, crossed, b)


def grid_to_tiles(blocks, swaps):
    pairs = [swap_halves(blocks[k], blocks[2 + k], 1) for k in (0, 1)]
    out = []
    for z in (0, 1):
        halves = swap_halves(pairs[0][z], pairs[1][z], 0)
        out.append([transpose_chunks(one, swaps) for one in halves])
    return out


def tiles_to_grid(tiles, swaps):
    pairs = []
    for z in (0, 1):
        a, b = (transpose_chunks(one, swaps) for one in tiles[z])
        pairs.append(swap_halves(a, b, 0))
    blocks = [None] * 4
    for k in (0, 1):
        blocks[k], blocks[2 + k] = swap_halves(pairs[0][k], pairs[1][k], 1)
    return blocks


def make_table(gas_ref, table_ref, part):
    swaps = chunk_swaps()
    flat_ref = table_ref.reshape(SLOTS * 4, 128)

    def step(n, carry):
        a, yo = n // 2, n % 2
        y0 = pl.multiple_of(yo * 8, 8)
        for h in (0, 1):
            for f in range(4):
                blocks = []
                for u in range(4):
                    part = gas_ref[f, a * 4 + u, pl.ds(y0, 8), pl.ds(h * 128, 128)]
                    if f == 3:
                        part = part - gas_ref[4, a * 4 + u, pl.ds(y0, 8), pl.ds(h * 128, 128)]
                    blocks.append(part)
                tiles = grid_to_tiles(blocks, swaps)
                for z in (0, 1):
                    for bh in (0, 1):
                        t0 = (a * 4 + yo * 2 + bh) * 32 + (h * 2 + z) * 8
                        flat_ref[pl.ds(t0 * 4 + f, 8, stride=4), :] = tiles[z][bh]
        return carry

    lax.fori_loop(2 * part, 2 * part + 2, step, 0)


def split_three(ref, g):
    low = rows() < 4
    v0, v1, v2 = (ref[pl.ds(pl.multiple_of(g * 24 + 8 * n, 8), 8), :] for n in range(3))
    middle = pltpu.roll(jnp.where(low, v2, v0), 4, 0)
    return jnp.where(low, v0, v1), middle, jnp.where(low, v1, v2)


def join_three(ref, g, f0, f1, f2):
    low = rows() < 4
    middle = pltpu.roll(f1, 4, 0)
    out = (jnp.where(low, f0, middle), jnp.where(low, f2, f0), jnp.where(low, middle, f2))
    for n in range(3):
        ref[pl.ds(pl.multiple_of(g * 24 + 8 * n, 8), 8), :] = out[n]


def parcels(g, count_ref, tiles_ref, speed_ref, mass_ref, offset_ref, cell_ref, speed_out, mass_out, lhs_ref, q_ref):
    low = rows() < 4
    cx, cy, cz = split_three(cell_ref, g)
    ox, oy, oz = split_three(offset_ref, g)
    speed = split_three(speed_ref, g)
    mass = mass_ref[pl.ds(pl.multiple_of(g * 8, 8), 8), :]
    q = cx * 32 + cy * 8 + cz
    wx, wy, wz = ((1.0 - o, o) for o in (ox, oy, oz))
    weights = []
    for u in (0, 1):
        for v in (0, 1):
            both = wx[u] * wy[v]
            weights += [both * wz[0], both * wz[1]]
    index = [q + shift for shift in SHIFTS]
    sampled = []
    for f in range(4):
        tile = tiles_ref[pl.ds(g * 32 + f, 8, stride=4), :]
        total = None
        for c in range(8):
            term = jnp.take_along_axis(tile, index[c], axis=1) * weights[c]
            total = term if total is None else total + term
        sampled.append(total)
    log_radius = jnp.log(mass) * (1.0 / 3.0)
    inverse_radius = jnp.exp(-log_radius)
    drag = DRAG_RATE * inverse_radius * inverse_radius
    live = (rows() % 4) < jnp.where(low, count_ref[2 * g], count_ref[2 * g + 1])
    scale = 1.0 / (1.0 + drag)
    gap = sampled[3]
    softplus = jnp.maximum(gap, 0.0) + jnp.log(1.0 + jnp.exp(-jnp.abs(gap)))
    mass_new = mass / (1.0 + EVAPORATION * softplus * inverse_radius)
    mass_new = jnp.where(live, mass_new, mass)
    vapour = mass - mass_new
    speed_new, source = [], []
    for f in range(3):
        moved = jnp.where(live, (speed[f] + drag * sampled[f]) * scale, speed[f])
        speed_new.append(moved)
        source.append(mass * (speed[f] - moved) + vapour * moved)
    source.append(vapour)
    join_three(speed_out, g, *speed_new)
    mass_out[pl.ds(pl.multiple_of(g * 8, 8), 8), :] = mass_new
    for f in range(4):
        value = jnp.where(live, source[f], 0.0)
        for c in range(8):
            lhs_ref[pl.ds(c * 32 + f, 8, stride=4), :] = value * weights[c]
    q_ref[...] = q


def deposits(g, lhs_ref, q_ref, out_ref):
    entry = lax.broadcasted_iota(I32, (128, 128), 0)
    first = lax.broadcasted_iota(I32, (64, 128), 0) % 8 < 4
    keep = jnp.where(first, 1.0, 0.0).astype(BF16)
    drop = jnp.where(first, 0.0, 1.0).astype(BF16)
    for j in range(4):
        left = jnp.concatenate([lhs_ref[pl.ds(c * 32 + j * 8, 8), :] for c in range(8)], axis=0)
        high = left.astype(BF16)
        rest = (left - high.astype(F32)).astype(BF16)
        left = jnp.concatenate(
            [
                jnp.concatenate([high * keep, high * drop], axis=1),
                jnp.concatenate([rest * keep, rest * drop], axis=1),
            ],
            axis=0,
        )
        hits = []
        for k in (0, 1):
            at = jnp.broadcast_to(q_ref[pl.ds(2 * j + k, 1), :], (128, 128))
            hits.append(jnp.where(at == entry, 1.0, 0.0).astype(BF16))
        right = jnp.concatenate(hits, axis=1)
        both = lax.dot_general(left, right, (((1,), (1,)), ((), ())), preferred_element_type=F32)
        both = both[:64] + both[64:]
        total = both[:8]
        for c in range(1, 8):
            total = total + pltpu.roll(both[c * 8 : c * 8 + 8], SHIFTS[c], 1)
        out_ref[pl.ds(pl.multiple_of(g * 32 + j * 8, 8), 8), :] = total


def place():
    gx, yz = lax.axis_index("gx"), lax.axis_index("yz")
    return lax.div(gx, 2), lax.rem(gx, 2), lax.div(yz, 4), lax.rem(yz, 4)


def choose(turn, values):
    if isinstance(turn, int):
        return values[turn]
    bit = 1
    while len(values) > 1:
        odd = lax.rem(lax.div(turn, bit), 2) == 1
        values = [a if isinstance(a, int) and isinstance(b, int) and a == b else jnp.where(odd, b, a) for a, b in zip(values[::2], values[1::2])]
        bit *= 2
    return values[0]


def pairs(turn, sign):
    y, core, x, z = place()
    out = []
    for n in range(4):
        oy, ox, oc, oz = (choose(turn, [one[n][part] for one in ORDER]) for part in range(4))
        gx = lax.rem(y + sign * oy + 4, 4) * 2 + lax.rem(core + oc, 2)
        out.append((gx, lax.rem(x + sign * ox + 4, 4) * 4 + lax.rem(lax.div(z, 2) + oz, 2) * 2))
    return out


def members(turn, sign):
    _, _, _, z = place()
    mine = lax.rem(z, 2)
    out = []
    for gx, yz in pairs(turn, sign):
        out += [(gx, yz + mine), (gx, yz + 1 - mine)]
    return out


def exchange_kernel(
    count_hbm, index_hbm, gas_hbm, speed_hbm, mass_hbm, offset_hbm, cell_hbm,
    speed_out, mass_out, arrived_ref, wanted_ref, base_ref,
    gas_ref, speed_ref, mass_ref, offset_ref, cell_ref, count_ref, index_ref,
    ask_ref, got_ref, smem_ref, table_ref, send_ref, tiles_ref, deposit_ref, lhs_ref, q_ref, edge_ref, halo_ref,
    near_sems, load_sems, move_sems, ask_sems, down_sems, tile_sems, edge_sems, halo_sems,
):
    gx, yz = lax.axis_index("gx"), lax.axis_index("yz")
    me = gx * 16 + yz
    barrier = pltpu.get_barrier_semaphore()

    def others(turn, sign, act):
        for n, to in enumerate(members(turn, sign)):
            one = functools.partial(act, to[0] * 16 + to[1], to)
            if n != SELF:
                one()
            elif isinstance(turn, int):
                if turn != HERE:
                    one()
            else:
                pl.when(turn != HERE)(one)

    loads = [
        pltpu.make_async_copy(src, dst, load_sems.at[n])
        for n, (src, dst) in enumerate(
            (
                (index_hbm, index_ref),
                (gas_hbm, gas_ref),
                (speed_hbm, speed_ref),
                (mass_hbm, mass_ref),
                (offset_hbm, offset_ref),
                (cell_hbm, cell_ref),
                (count_hbm, count_ref),
            )
        )
    ]
    for load in loads:
        load.start()
    y, core, x, z = place()
    beside = [
        (lax.rem(y + step, 4) * 2 + core, lax.rem(x + other, 4) * 4 + z)
        for step, other in ((1, 0), (3, 0), (0, 1), (0, 3))
    ]
    mates = [(y * 2 + lax.rem(core + n // 4, 2), x * 4 + lax.rem(z + n, 4)) for n in range(1, 8)]
    for to in mates + beside:
        pl.semaphore_signal(barrier, inc=1, device_id=to, device_id_type=MESH)
    def move(src, dst, sem, to, arrival=None):
        return pltpu.make_async_remote_copy(
            src_ref=src,
            dst_ref=dst,
            send_sem=move_sems.at[sem],
            recv_sem=move_sems.at[sem + 1] if arrival is None else arrival,
            device_id=to,
            device_id_type=MESH,
        )

    partner = (gx, lax.rem(yz + 1, 16))

    def ask(turn):
        others(turn, 1, lambda d, to: move(ask_ref.at[d], got_ref.at[me], 0, to, ask_sems.at[turn]).start())

    def ask_turns(turns):
        for turn in range(*turns):
            ask(turn)

    pl.semaphore_wait(barrier, len(mates + beside))
    for n, turns in enumerate(REACH):
        if n < 4:
            for to in beside:
                pl.semaphore_signal(near_sems.at[n], inc=1, device_id=to, device_id_type=MESH)
        if n == 0:
            loads[0].wait()
            ask_ref[:, 0, :] = jnp.concatenate([index_ref[...], jnp.zeros((124, 128), I32)], axis=0).T
            got_ref[me] = ask_ref[me]
            loads[1].wait()
        if n < 4:
            make_table(gas_ref, table_ref, n)
        ask_turns(turns)
        if n == 1:
            ask_turns(LATE)
        if n < 4:
            pl.semaphore_wait(near_sems.at[n], len(beside))
    make_edges(gas_ref, edge_ref)

    halos = []
    for n, (here, there, to) in enumerate(
        (
            (gx < 7, gx > 0, (gx + 1, yz)),
            (gx > 0, gx < 7, (gx - 1, yz)),
            (yz < 15, yz > 0, (gx, yz + 1)),
            (yz > 0, yz < 15, (gx, yz - 1)),
        )
    ):
        halo = pltpu.make_async_remote_copy(
            src_ref=edge_ref.at[n],
            dst_ref=halo_ref.at[n],
            send_sem=edge_sems.at[n],
            recv_sem=halo_sems.at[n],
            device_id=to,
            device_id_type=MESH,
        )
        halos.append((here, there, halo))

    def start_halos():
        for n, (here, there, halo) in enumerate(halos):
            pl.when(here)(halo.start)

            @pl.when(jnp.logical_not(there))
            def _(n=n):
                halo_ref[n] = jnp.zeros(halo_ref.shape[1:], F32)

    start_halos()

    def await_turn(turn, sem, src, dst, per_device):
        def wait(devices):
            every = pl.ds(0, devices * per_device)
            move(src.at[every], dst.at[every], sem[0], partner, sem[1].at[turn]).wait_recv()

        pl.when(turn == HERE)(lambda: wait(7))
        pl.when(turn != HERE)(lambda: wait(8))

    def start_down(turn):
        await_turn(turn, (0, ask_sems), ask_ref, got_ref, 1)
        for to in pairs(turn, -1):
            part = pl.ds(to[0] * 16 + to[1], 2)
            pltpu.make_async_copy(got_ref.at[part], smem_ref.at[part], down_sems.at[turn]).start()

    def await_down(turn):
        part = pl.ds(0, 8)
        pltpu.make_async_copy(got_ref.at[part], smem_ref.at[part], down_sems.at[turn]).wait()

    def block(ref, d):
        return ref.at[pl.ds(pl.multiple_of(d * 16, 16), 16)]

    def pick(d, dst):
        for k in range(4):
            dst[pl.ds(pl.multiple_of(d * 16 + k * 4, 4), 4), :] = table_ref[smem_ref[d, 0, k]]

    def pick_turn(turn):
        await_down(turn)
        others(turn, -1, lambda d, to: pick(d, send_ref))

    def send_turn(turn):
        others(
            turn,
            -1,
            lambda d, to: move(block(send_ref, d), block(tiles_ref, me), 2, to, tile_sems.at[turn]).start(),
        )

    def pick_step(turn, carry):
        pl.when(turn < TURNS - 1)(lambda: start_down(turn + 1))
        pick_turn(turn)
        send_turn(turn - 1)
        return carry

    start_down(0)
    start_down(1)
    pick_turn(0)
    pick(me, tiles_ref)
    lax.fori_loop(1, TURNS, pick_step, 0)
    send_turn(TURNS - 1)
    wanted_ref[...] = got_ref[:, 0, :].T[:8]

    for load in loads[2:]:
        load.wait()
    for here, there, halo in halos:
        pl.when(there)(halo.wait_recv)
    diffuse(gas_ref, halo_ref, base_ref)

    def await_tiles(turn):
        await_turn(turn, (2, tile_sems), send_ref, tiles_ref, 16)

    def groups(turn):
        return [to[0] * 8 + lax.div(to[1], 2) for to in pairs(turn, 1)]

    def first(turn):
        for n, g in enumerate(groups(turn)):
            parcels(g, count_ref, tiles_ref, speed_ref, mass_ref, offset_ref, cell_ref, speed_out, mass_out, lhs_ref.at[n], q_ref.at[n])

    def second(turn):
        for n, g in enumerate(groups(turn)):
            deposits(g, lhs_ref.at[n], q_ref.at[n], deposit_ref)

    def give(turn):
        others(turn, 1, lambda d, to: move(block(deposit_ref, d), block(arrived_ref, me), 3, to).start())

    def step(turn, carry):
        await_tiles(turn)
        second(turn - 1)
        first(turn)
        pl.when(turn > 1)(lambda: give(turn - 2))
        return carry

    await_tiles(0)
    first(0)
    lax.fori_loop(1, TURNS, step, 0)
    give(TURNS - 2)
    second(TURNS - 1)
    mine = pl.ds(pl.multiple_of(me * 16, 16), 16)
    arrived_ref[mine, :] = deposit_ref[mine, :]
    give(TURNS - 1)

    rest = pl.ds(0, DEVICES - 1)
    move(ask_ref.at[rest], got_ref.at[rest], 0, partner).wait_send()
    for here, there, halo in halos:
        pl.when(here)(halo.wait_send)
    rest = pl.ds(0, (DEVICES - 1) * 16)
    move(send_ref.at[rest], tiles_ref.at[rest], 2, partner).wait_send()
    gifts = move(deposit_ref.at[rest], arrived_ref.at[rest], 3, partner)
    gifts.wait_send()
    gifts.wait_recv()


def make_edges(gas_ref, edge_ref):
    def step(f, carry):
        edge_ref[0, f] = gas_ref[f, 15]
        edge_ref[1, f] = gas_ref[f, 0]
        for x in range(16):
            edge_ref[2, f, x : x + 1, :] = gas_ref[f, x, 15:16, :]
            edge_ref[3, f, x : x + 1, :] = gas_ref[f, x, 0:1, :]
        return carry

    lax.fori_loop(0, 5, step, 0)


def spread(plane_ref, f, x, xs, halos):
    xlo, xhi, ylo, yhi = halos
    value = plane_ref[f, x]
    row = lax.broadcasted_iota(I32, value.shape, 0)
    lane = lax.broadcasted_iota(I32, value.shape, 1)
    ny, nz = value.shape
    below = xlo[f] if x == 0 else plane_ref[f, x - 1]
    above = xhi[f] if x == xs - 1 else plane_ref[f, x + 1]
    total = below + above
    total = total + jnp.where(row == 0, ylo[f, x : x + 1, :], pltpu.roll(value, 1, 0))
    total = total + jnp.where(row == ny - 1, yhi[f, x : x + 1, :], pltpu.roll(value, ny - 1, 0))
    total = total + jnp.where(lane == 0, 0.0, pltpu.roll(value, 1, 1))
    total = total + jnp.where(lane == nz - 1, 0.0, pltpu.roll(value, nz - 1, 1))
    return value + DIFFUSION * (total - 6.0 * value)


def diffuse(gas_ref, halo_ref, out_ref):
    xs = gas_ref.shape[1]

    def step(f, carry):
        for x in range(xs):
            out_ref[f, x] = spread(gas_ref, f, x, xs, [halo_ref.at[n] for n in range(4)])
        return carry

    lax.fori_loop(0, gas_ref.shape[0], step, 0)


def finish_kernel(base_ref, wanted_ref, arrived_ref, speed_ref, mass_ref, out_hbm, speed_hbm, mass_hbm, out_ref, sum_ref, hit_ref, sems):
    stores = [
        pltpu.make_async_copy(speed_ref, speed_hbm, sems.at[0]),
        pltpu.make_async_copy(mass_ref, mass_hbm, sems.at[1]),
    ]
    for store in stores:
        store.start()
    lane = lanes()
    for part in range(4):
        at = None
        for k in range(4):
            row = jnp.broadcast_to(wanted_ref[pl.ds(k, 1), :], (8, 128))
            mine = jnp.take_along_axis(row, part * 32 + lane // 4, axis=1)
            at = mine if at is None else jnp.where(lane % 4 == k, mine, at)
        at = jnp.broadcast_to(at[:1], (512, 128))
        tile = lax.broadcasted_iota(I32, (512, 128), 0)
        hit_ref[:, pl.ds(part * 128, 128)] = jnp.where(at == tile, 1.0, 0.0).astype(BF16)
    swaps = chunk_swaps()

    def add_up(f):
        value = arrived_ref[pl.ds(f, 512, stride=4), :]
        high = value.astype(BF16)
        rest = (value - high.astype(F32)).astype(BF16)
        both = jnp.concatenate([high, rest], axis=1)
        both = jnp.dot(hit_ref[...], both, preferred_element_type=F32)
        sum_ref[f] = both[:, :128] + both[:, 128:]

    def lay_out(f, a, yo, h):
        tiles = []
        for z in (0, 1):
            tiles.append([])
            for bh in (0, 1):
                t0 = (a * 4 + yo * 2 + bh) * 32 + (h * 2 + z) * 8
                tiles[z].append(sum_ref[f, pl.ds(t0, 8), :])
        blocks = tiles_to_grid(tiles, swaps)
        for u in range(4):
            at = (a * 4 + u, pl.ds(yo * 8, 8), pl.ds(h * 128, 128))
            add = blocks[u] * (1.0 / CELL_MASS)
            if f < 3:
                out_ref[f, *at] = base_ref[f, *at] + add
            else:
                out_ref[3, *at] = base_ref[3, *at] - LATENT_HEAT * add
                out_ref[4, *at] = base_ref[4, *at] + add

    order = (3, 0, 1, 2)
    add_up(order[0])
    for n, f in enumerate(order):
        if n < 3:
            add_up(order[n + 1])
        for a in range(4):
            for yo in (0, 1):
                for h in (0, 1):
                    lay_out(f, a, yo, h)
        for field in (3, 4) if f == 3 else (f,):
            store = pltpu.make_async_copy(out_ref.at[field], out_hbm.at[field], sems.at[2 + field])
            store.start()
            stores.append(store)
    for store in stores:
        store.wait()


VMEM = pl.BlockSpec(memory_space=pltpu.VMEM)
SMEM = pl.BlockSpec(memory_space=pltpu.SMEM)
HBM = pl.BlockSpec(memory_space=pltpu.HBM)


def call(kernel, name, out, in_specs, out_specs, scratch=(), limit=48, **params):
    return pl.pallas_call(
        kernel,
        name=name,
        out_shape=out,
        in_specs=in_specs,
        out_specs=out_specs,
        scratch_shapes=scratch,
        compiler_params=pltpu.CompilerParams(vmem_limit_bytes=limit * 1024 * 1024, **params),
    )


def array(*shape, dtype=F32):
    return jax.ShapeDtypeStruct(shape, dtype)


def shards(gas_state, parcel_speed, parcel_mass, offsets, cell_base, block_tile, block_count):
    def three(value):
        return value.reshape(DEVICES, 4, 3, 128).transpose(0, 2, 1, 3).reshape(SLOTS * 3, 128)

    def hbm(value):
        return pltpu.with_memory_space_constraint(value, pltpu.HBM)

    dma = pltpu.SemaphoreType.DMA
    parcel_outs = (array(SLOTS * 3, 128), array(SLOTS, 128))
    grid = array(*gas_state.shape)
    edge = (4, 5, 16, 256)
    speed_next, mass_next, arrived, wanted, base = call(
        exchange_kernel,
        "exchange",
        parcel_outs + (array(SLOTS * 4, 128), array(8, 128, dtype=I32), grid),
        [HBM] * 7,
        (VMEM,) * 5,
        [
            pltpu.VMEM(gas_state.shape, F32),
            pltpu.VMEM((SLOTS * 3, 128), F32),
            pltpu.VMEM((SLOTS, 128), F32),
            pltpu.VMEM((SLOTS * 3, 128), F32),
            pltpu.VMEM((SLOTS * 3, 128), I32),
            pltpu.SMEM((DEVICES,), I32),
            pltpu.VMEM((4, DEVICES), I32),
            pltpu.VMEM((DEVICES, 1, 128), I32),
            pltpu.VMEM((DEVICES, 1, 128), I32),
            pltpu.SMEM((DEVICES, 1, 128), I32),
            pltpu.VMEM((SLOTS, 4, 128), F32),
            pltpu.VMEM((SLOTS * 4, 128), F32),
            pltpu.VMEM((SLOTS * 4, 128), F32),
            pltpu.VMEM((SLOTS * 4, 128), F32),
            pltpu.VMEM((4, 256, 128), F32),
            pltpu.VMEM((4, 8, 128), I32),
            pltpu.VMEM(edge, F32),
            pltpu.VMEM(edge, F32),
            pltpu.SemaphoreType.REGULAR((4,)),
            dma((7,)),
            dma((5,)),
            dma((TURNS,)),
            dma((TURNS,)),
            dma((TURNS,)),
            dma((4,)),
            dma((4,)),
        ],
        limit=48,
        collective_id=0,
        has_side_effects=True,
    )(
        hbm(block_count.reshape(DEVICES)),
        hbm(block_tile.reshape(DEVICES, 4).T),
        hbm(gas_state),
        hbm(three(parcel_speed)),
        hbm(parcel_mass.reshape(SLOTS, 128)),
        hbm(three(offsets)),
        hbm(three(cell_base)),
    )
    gas_next, speed_next, mass_next = call(
        finish_kernel,
        "finish",
        (grid,) + parcel_outs,
        [VMEM] * 5,
        (HBM,) * 3,
        [
            pltpu.VMEM(gas_state.shape, F32),
            pltpu.VMEM((4, SLOTS, 128), F32),
            pltpu.VMEM((SLOTS, SLOTS), BF16),
            dma((7,)),
        ],
    )(base, wanted, arrived, speed_next, mass_next)
    speed_next = speed_next.reshape(DEVICES, 3, 4, 128).transpose(0, 2, 1, 3)
    return gas_next, speed_next.reshape(parcel_speed.shape), mass_next.reshape(parcel_mass.shape)


def solution(mesh):
    in_specs = (
        P(None, "gx", "yz", None),
        P("gx", "yz", None, None, None, None),
        P("gx", "yz", None, None, None),
        P("gx", "yz", None, None, None, None),
        P("gx", "yz", None, None, None, None),
        P("gx", "yz", None, None),
        P("gx", "yz", None),
    )
    out_specs = (
        P(None, "gx", "yz", None),
        P("gx", "yz", None, None, None, None),
        P("gx", "yz", None, None, None),
    )
    return jax.shard_map(shards, mesh=mesh, in_specs=in_specs, out_specs=out_specs, check_vma=False)
```

```python
import functools

import jax
import jax.numpy as jnp
from jax import lax
from jax.experimental import pallas as pl
from jax.experimental.pallas import tpu as pltpu
from jax.sharding import PartitionSpec as P

F32 = jnp.float32
BF16 = jnp.bfloat16
I32 = jnp.int32
MESH = pl.DeviceIdType.MESH

DIFFUSION = 0.1
CELL_MASS = 4.0
DRAG_RATE = 0.5
EVAPORATION = 0.3
LATENT_HEAT = 2.0

SHIFTS = (0, 1, 8, 9, 32, 33, 40, 41)

DEVICES = 128
SLOTS = 512


def turn_list():
    rings = {
        "near": ((1, 0), (3, 0), (0, 1), (0, 3)),
        "side": ((1, 1), (3, 3), (1, 3), (3, 1)),
        "long": ((2, 1), (2, 3), (1, 2), (3, 2)),
    }
    flags = ((1, 1), (0, 1), (1, 0), (0, 0))
    here = [(0, 0, *flag) for flag in flags]
    far = [(2, 2, *flag) for flag in flags]

    def ring(name, core, z):
        return [(y, x, core, z) for y, x in rings[name]]

    def half(core):
        return [(2, 0, core, 0), (0, 2, core, 0), (2, 0, core, 1), (0, 2, core, 1)]

    return (
        here,
        ring("near", 0, 0),
        ring("near", 1, 1),
        ring("side", 0, 0),
        half(0),
        ring("side", 1, 1),
        half(1),
        ring("side", 0, 1),
        ring("side", 1, 0),
        ring("long", 0, 0),
        ring("long", 1, 1),
        ring("long", 0, 1),
        ring("long", 1, 0),
        far,
        ring("near", 0, 1),
        ring("near", 1, 0),
    )


ORDER = turn_list()
TURNS = len(ORDER)
REACH = ((0, 1), (1, 3), (3, 9), (9, 13), (13, 14))
LATE = (14, 16)
HERE, SELF = 0, 3


def lanes():
    return lax.broadcasted_iota(I32, (8, 128), 1)


def rows():
    return lax.broadcasted_iota(I32, (8, 128), 0)


def chunk_swaps():
    row, lane = rows(), lanes()
    half, chunk, rest = lane // 64, (lane // 8) % 8, lane % 8
    first = half * 64 + ((chunk - row) % 8) * 8 + rest
    second = (chunk - row) % 8
    third = half * 64 + ((chunk + row) % 8) * 8 + rest
    return first, second, third


def transpose_chunks(block, swaps):
    first, second, third = swaps
    block = jnp.take_along_axis(block, first, axis=1)
    block = jnp.take_along_axis(block, second, axis=0)
    return jnp.take_along_axis(block, third, axis=1)


def swap_halves(a, b, axis):
    size = a.shape[axis] // 2
    low = (lanes() < 64) if axis == 1 else (rows() < 4)
    crossed = pltpu.roll(jnp.where(low, b, a), size, axis)
    return jnp.where(low, a, crossed), jnp.where(low, crossed, b)


def grid_to_tiles(blocks, swaps):
    pairs = [swap_halves(blocks[k], blocks[2 + k], 1) for k in (0, 1)]
    out = []
    for z in (0, 1):
        halves = swap_halves(pairs[0][z], pairs[1][z], 0)
        out.append([transpose_chunks(one, swaps) for one in halves])
    return out


def tiles_to_grid(tiles, swaps):
    pairs = []
    for z in (0, 1):
        a, b = (transpose_chunks(one, swaps) for one in tiles[z])
        pairs.append(swap_halves(a, b, 0))
    blocks = [None] * 4
    for k in (0, 1):
        blocks[k], blocks[2 + k] = swap_halves(pairs[0][k], pairs[1][k], 1)
    return blocks


def make_table(gas_ref, table_ref, part):
    swaps = chunk_swaps()
    flat_ref = table_ref.reshape(SLOTS * 4, 128)

    def step(n, carry):
        a, yo = n // 2, n % 2
        y0 = pl.multiple_of(yo * 8, 8)
        for h in (0, 1):
            for f in range(4):
                blocks = []
                for u in range(4):
                    part = gas_ref[f, a * 4 + u, pl.ds(y0, 8), pl.ds(h * 128, 128)]
                    if f == 3:
                        part = part - gas_ref[4, a * 4 + u, pl.ds(y0, 8), pl.ds(h * 128, 128)]
                    blocks.append(part)
                tiles = grid_to_tiles(blocks, swaps)
                for z in (0, 1):
                    for bh in (0, 1):
                        t0 = (a * 4 + yo * 2 + bh) * 32 + (h * 2 + z) * 8
                        flat_ref[pl.ds(t0 * 4 + f, 8, stride=4), :] = tiles[z][bh]
        return carry

    lax.fori_loop(2 * part, 2 * part + 2, step, 0)


def split_three(ref, g):
    low = rows() < 4
    v0, v1, v2 = (ref[pl.ds(pl.multiple_of(g * 24 + 8 * n, 8), 8), :] for n in range(3))
    middle = pltpu.roll(jnp.where(low, v2, v0), 4, 0)
    return jnp.where(low, v0, v1), middle, jnp.where(low, v1, v2)


def join_three(ref, g, f0, f1, f2):
    low = rows() < 4
    middle = pltpu.roll(f1, 4, 0)
    out = (jnp.where(low, f0, middle), jnp.where(low, f2, f0), jnp.where(low, middle, f2))
    for n in range(3):
        ref[pl.ds(pl.multiple_of(g * 24 + 8 * n, 8), 8), :] = out[n]


def parcels(g, count_ref, tiles_ref, speed_ref, mass_ref, offset_ref, cell_ref, speed_out, mass_out, lhs_ref, q_ref):
    low = rows() < 4
    cx, cy, cz = split_three(cell_ref, g)
    ox, oy, oz = split_three(offset_ref, g)
    speed = split_three(speed_ref, g)
    mass = mass_ref[pl.ds(pl.multiple_of(g * 8, 8), 8), :]
    q = cx * 32 + cy * 8 + cz
    wx, wy, wz = ((1.0 - o, o) for o in (ox, oy, oz))
    weights = []
    for u in (0, 1):
        for v in (0, 1):
            both = wx[u] * wy[v]
            weights += [both * wz[0], both * wz[1]]
    index = [q + shift for shift in SHIFTS]
    sampled = []
    for f in range(4):
        tile = tiles_ref[pl.ds(g * 32 + f, 8, stride=4), :]
        total = None
        for c in range(8):
            term = jnp.take_along_axis(tile, index[c], axis=1) * weights[c]
            total = term if total is None else total + term
        sampled.append(total)
    log_radius = jnp.log(mass) * (1.0 / 3.0)
    inverse_radius = jnp.exp(-log_radius)
    drag = DRAG_RATE * inverse_radius * inverse_radius
    live = (rows() % 4) < jnp.where(low, count_ref[2 * g], count_ref[2 * g + 1])
    scale = 1.0 / (1.0 + drag)
    gap = sampled[3]
    softplus = jnp.maximum(gap, 0.0) + jnp.log(1.0 + jnp.exp(-jnp.abs(gap)))
    mass_new = mass / (1.0 + EVAPORATION * softplus * inverse_radius)
    mass_new = jnp.where(live, mass_new, mass)
    vapour = mass - mass_new
    speed_new, source = [], []
    for f in range(3):
        moved = jnp.where(live, (speed[f] + drag * sampled[f]) * scale, speed[f])
        speed_new.append(moved)
        source.append(mass * (speed[f] - moved) + vapour * moved)
    source.append(vapour)
    join_three(speed_out, g, *speed_new)
    mass_out[pl.ds(pl.multiple_of(g * 8, 8), 8), :] = mass_new
    for f in range(4):
        value = jnp.where(live, source[f], 0.0)
        for c in range(8):
            lhs_ref[pl.ds(c * 32 + f, 8, stride=4), :] = value * weights[c]
    q_ref[...] = q


def deposits(g, lhs_ref, q_ref, out_ref):
    entry = lax.broadcasted_iota(I32, (128, 128), 0)
    first = lax.broadcasted_iota(I32, (64, 128), 0) % 8 < 4
    keep = jnp.where(first, 1.0, 0.0).astype(BF16)
    drop = jnp.where(first, 0.0, 1.0).astype(BF16)
    for j in range(4):
        left = jnp.concatenate([lhs_ref[pl.ds(c * 32 + j * 8, 8), :] for c in range(8)], axis=0)
        high = left.astype(BF16)
        rest = (left - high.astype(F32)).astype(BF16)
        left = jnp.concatenate(
            [
                jnp.concatenate([high * keep, high * drop], axis=1),
                jnp.concatenate([rest * keep, rest * drop], axis=1),
            ],
            axis=0,
        )
        hits = []
        for k in (0, 1):
            at = jnp.broadcast_to(q_ref[pl.ds(2 * j + k, 1), :], (128, 128))
            hits.append(jnp.where(at == entry, 1.0, 0.0).astype(BF16))
        right = jnp.concatenate(hits, axis=1)
        both = lax.dot_general(left, right, (((1,), (1,)), ((), ())), preferred_element_type=F32)
        both = both[:64] + both[64:]
        total = both[:8]
        for c in range(1, 8):
            total = total + pltpu.roll(both[c * 8 : c * 8 + 8], SHIFTS[c], 1)
        out_ref[pl.ds(pl.multiple_of(g * 32 + j * 8, 8), 8), :] = total


def place():
    gx, yz = lax.axis_index("gx"), lax.axis_index("yz")
    return lax.div(gx, 2), lax.rem(gx, 2), lax.div(yz, 4), lax.rem(yz, 4)


def choose(turn, values):
    if isinstance(turn, int):
        return values[turn]
    bit = 1
    while len(values) > 1:
        odd = lax.rem(lax.div(turn, bit), 2) == 1
        values = [a if isinstance(a, int) and isinstance(b, int) and a == b else jnp.where(odd, b, a) for a, b in zip(values[::2], values[1::2])]
        bit *= 2
    return values[0]


def pairs(turn, sign):
    y, core, x, z = place()
    out = []
    for n in range(4):
        oy, ox, oc, oz = (choose(turn, [one[n][part] for one in ORDER]) for part in range(4))
        gx = lax.rem(y + sign * oy + 4, 4) * 2 + lax.rem(core + oc, 2)
        out.append((gx, lax.rem(x + sign * ox + 4, 4) * 4 + lax.rem(lax.div(z, 2) + oz, 2) * 2))
    return out


def members(turn, sign):
    _, _, _, z = place()
    mine = lax.rem(z, 2)
    both = pairs(turn, sign)
    return [(gx, yz + mine) for gx, yz in both] + [(gx, yz + 1 - mine) for gx, yz in both]


def exchange_kernel(
    count_hbm, index_hbm, gas_hbm, speed_hbm, mass_hbm, offset_hbm, cell_hbm,
    speed_out, mass_out, arrived_ref, wanted_ref, base_ref,
    gas_ref, speed_ref, mass_ref, offset_ref, cell_ref, count_ref, index_ref,
    ask_ref, got_ref, smem_ref, table_ref, send_ref, tiles_ref, deposit_ref, lhs_ref, q_ref, edge_ref, halo_ref,
    near_sems, load_sems, move_sems, ask_sems, down_sems, tile_sems, edge_sems, halo_sems,
):
    gx, yz = lax.axis_index("gx"), lax.axis_index("yz")
    me = gx * 16 + yz
    barrier = pltpu.get_barrier_semaphore()

    def others(turn, sign, act):
        for n, to in enumerate(members(turn, sign)):
            one = functools.partial(act, to[0] * 16 + to[1], to)
            if n != SELF:
                one()
            elif isinstance(turn, int):
                if turn != HERE:
                    one()
            else:
                pl.when(turn != HERE)(one)

    loads = [
        pltpu.make_async_copy(src, dst, load_sems.at[n])
        for n, (src, dst) in enumerate(
            (
                (index_hbm, index_ref),
                (gas_hbm, gas_ref),
                (speed_hbm, speed_ref),
                (mass_hbm, mass_ref),
                (offset_hbm, offset_ref),
                (cell_hbm, cell_ref),
                (count_hbm, count_ref),
            )
        )
    ]
    for load in loads:
        load.start()
    y, core, x, z = place()
    beside = [
        (lax.rem(y + step, 4) * 2 + core, lax.rem(x + other, 4) * 4 + z)
        for step, other in ((1, 0), (3, 0), (0, 1), (0, 3))
    ]
    mates = [(y * 2 + lax.rem(core + n // 4, 2), x * 4 + lax.rem(z + n, 4)) for n in range(1, 8)]
    for to in mates + beside:
        pl.semaphore_signal(barrier, inc=1, device_id=to, device_id_type=MESH)
    def move(src, dst, sem, to, arrival=None):
        return pltpu.make_async_remote_copy(
            src_ref=src,
            dst_ref=dst,
            send_sem=move_sems.at[sem],
            recv_sem=move_sems.at[sem + 1] if arrival is None else arrival,
            device_id=to,
            device_id_type=MESH,
        )

    partner = (gx, lax.rem(yz + 1, 16))

    def ask(turn):
        others(turn, 1, lambda d, to: move(ask_ref.at[d], got_ref.at[me], 0, to, ask_sems.at[turn]).start())

    def ask_turns(turns):
        for turn in range(*turns):
            ask(turn)

    pl.semaphore_wait(barrier, len(mates + beside))
    for n, turns in enumerate(REACH):
        if n < 4:
            for to in beside:
                pl.semaphore_signal(near_sems.at[n], inc=1, device_id=to, device_id_type=MESH)
        if n == 0:
            loads[0].wait()
            ask_ref[:, 0, :] = jnp.concatenate([index_ref[...], jnp.zeros((124, 128), I32)], axis=0).T
            got_ref[me] = ask_ref[me]
            loads[1].wait()
            make_table(gas_ref, table_ref, 0)
        ask_turns(turns)
        if n == 1:
            ask_turns(LATE)
        if 0 < n < 4:
            make_table(gas_ref, table_ref, n)
        if n < 4:
            pl.semaphore_wait(near_sems.at[n], len(beside))
    make_edges(gas_ref, edge_ref)

    halos = []
    for n, (here, there, to) in enumerate(
        (
            (gx < 7, gx > 0, (gx + 1, yz)),
            (gx > 0, gx < 7, (gx - 1, yz)),
            (yz < 15, yz > 0, (gx, yz + 1)),
            (yz > 0, yz < 15, (gx, yz - 1)),
        )
    ):
        halo = pltpu.make_async_remote_copy(
            src_ref=edge_ref.at[n],
            dst_ref=halo_ref.at[n],
            send_sem=edge_sems.at[n],
            recv_sem=halo_sems.at[n],
            device_id=to,
            device_id_type=MESH,
        )
        halos.append((here, there, halo))

    def start_halos():
        for n, (here, there, halo) in enumerate(halos):
            pl.when(here)(halo.start)

            @pl.when(jnp.logical_not(there))
            def _(n=n):
                halo_ref[n] = jnp.zeros(halo_ref.shape[1:], F32)

    start_halos()

    def await_turn(turn, sem, src, dst, per_device):
        def wait(devices):
            every = pl.ds(0, devices * per_device)
            move(src.at[every], dst.at[every], sem[0], partner, sem[1].at[turn]).wait_recv()

        pl.when(turn == HERE)(lambda: wait(7))
        pl.when(turn != HERE)(lambda: wait(8))

    def start_down(turn):
        await_turn(turn, (0, ask_sems), ask_ref, got_ref, 1)
        for to in pairs(turn, -1):
            part = pl.ds(to[0] * 16 + to[1], 2)
            pltpu.make_async_copy(got_ref.at[part], smem_ref.at[part], down_sems.at[turn]).start()

    def await_down(turn):
        part = pl.ds(0, 8)
        pltpu.make_async_copy(got_ref.at[part], smem_ref.at[part], down_sems.at[turn]).wait()

    def block(ref, d):
        return ref.at[pl.ds(pl.multiple_of(d * 16, 16), 16)]

    def pick(d, dst):
        for k in range(4):
            dst[pl.ds(pl.multiple_of(d * 16 + k * 4, 4), 4), :] = table_ref[smem_ref[d, 0, k]]

    def pick_turn(turn):
        await_down(turn)
        others(turn, -1, lambda d, to: pick(d, send_ref))

    def send_turn(turn):
        others(
            turn,
            -1,
            lambda d, to: move(block(send_ref, d), block(tiles_ref, me), 2, to, tile_sems.at[turn]).start(),
        )

    def pick_step(turn, carry):
        pl.when(turn < TURNS - 1)(lambda: start_down(turn + 1))
        pick_turn(turn)
        send_turn(turn - 1)
        return carry

    start_down(0)
    start_down(1)
    pick_turn(0)
    pick(me, tiles_ref)
    lax.fori_loop(1, TURNS, pick_step, 0)
    send_turn(TURNS - 1)
    wanted_ref[...] = got_ref[:, 0, :].T[:8]

    for load in loads[2:]:
        load.wait()
    for here, there, halo in halos:
        pl.when(there)(halo.wait_recv)
    diffuse(gas_ref, halo_ref, base_ref)

    def await_tiles(turn):
        await_turn(turn, (2, tile_sems), send_ref, tiles_ref, 16)

    def groups(turn):
        return [to[0] * 8 + lax.div(to[1], 2) for to in pairs(turn, 1)]

    def first(turn):
        for n, g in enumerate(groups(turn)):
            parcels(g, count_ref, tiles_ref, speed_ref, mass_ref, offset_ref, cell_ref, speed_out, mass_out, lhs_ref.at[n], q_ref.at[n])

    def second(turn):
        for n, g in enumerate(groups(turn)):
            deposits(g, lhs_ref.at[n], q_ref.at[n], deposit_ref)

    def give(turn):
        others(turn, 1, lambda d, to: move(block(deposit_ref, d), block(arrived_ref, me), 3, to).start())

    def step(turn, carry):
        await_tiles(turn)
        second(turn - 1)
        first(turn)
        pl.when(turn > 1)(lambda: give(turn - 2))
        return carry

    await_tiles(0)
    first(0)
    lax.fori_loop(1, TURNS, step, 0)
    give(TURNS - 2)
    second(TURNS - 1)
    mine = pl.ds(pl.multiple_of(me * 16, 16), 16)
    arrived_ref[mine, :] = deposit_ref[mine, :]
    give(TURNS - 1)

    rest = pl.ds(0, DEVICES - 1)
    move(ask_ref.at[rest], got_ref.at[rest], 0, partner).wait_send()
    for here, there, halo in halos:
        pl.when(here)(halo.wait_send)
    rest = pl.ds(0, (DEVICES - 1) * 16)
    move(send_ref.at[rest], tiles_ref.at[rest], 2, partner).wait_send()
    gifts = move(deposit_ref.at[rest], arrived_ref.at[rest], 3, partner)
    gifts.wait_send()
    gifts.wait_recv()


def make_edges(gas_ref, edge_ref):
    def step(f, carry):
        edge_ref[0, f] = gas_ref[f, 15]
        edge_ref[1, f] = gas_ref[f, 0]
        for x in range(16):
            edge_ref[2, f, x : x + 1, :] = gas_ref[f, x, 15:16, :]
            edge_ref[3, f, x : x + 1, :] = gas_ref[f, x, 0:1, :]
        return carry

    lax.fori_loop(0, 5, step, 0)


def spread(plane_ref, f, x, xs, halos):
    xlo, xhi, ylo, yhi = halos
    value = plane_ref[f, x]
    row = lax.broadcasted_iota(I32, value.shape, 0)
    lane = lax.broadcasted_iota(I32, value.shape, 1)
    ny, nz = value.shape
    below = xlo[f] if x == 0 else plane_ref[f, x - 1]
    above = xhi[f] if x == xs - 1 else plane_ref[f, x + 1]
    total = below + above
    total = total + jnp.where(row == 0, ylo[f, x : x + 1, :], pltpu.roll(value, 1, 0))
    total = total + jnp.where(row == ny - 1, yhi[f, x : x + 1, :], pltpu.roll(value, ny - 1, 0))
    total = total + jnp.where(lane == 0, 0.0, pltpu.roll(value, 1, 1))
    total = total + jnp.where(lane == nz - 1, 0.0, pltpu.roll(value, nz - 1, 1))
    return value + DIFFUSION * (total - 6.0 * value)


def diffuse(gas_ref, halo_ref, out_ref):
    xs = gas_ref.shape[1]

    def step(f, carry):
        for x in range(xs):
            out_ref[f, x] = spread(gas_ref, f, x, xs, [halo_ref.at[n] for n in range(4)])
        return carry

    lax.fori_loop(0, gas_ref.shape[0], step, 0)


def finish_kernel(base_ref, wanted_ref, arrived_ref, speed_ref, mass_ref, out_hbm, speed_hbm, mass_hbm, out_ref, sum_ref, hit_ref, sems):
    stores = [
        pltpu.make_async_copy(speed_ref, speed_hbm, sems.at[0]),
        pltpu.make_async_copy(mass_ref, mass_hbm, sems.at[1]),
    ]
    for store in stores:
        store.start()
    lane = lanes()
    for part in range(4):
        at = None
        for k in range(4):
            row = jnp.broadcast_to(wanted_ref[pl.ds(k, 1), :], (8, 128))
            mine = jnp.take_along_axis(row, part * 32 + lane // 4, axis=1)
            at = mine if at is None else jnp.where(lane % 4 == k, mine, at)
        at = jnp.broadcast_to(at[:1], (512, 128))
        tile = lax.broadcasted_iota(I32, (512, 128), 0)
        hit_ref[:, pl.ds(part * 128, 128)] = jnp.where(at == tile, 1.0, 0.0).astype(BF16)
    swaps = chunk_swaps()

    def add_up(f):
        value = arrived_ref[pl.ds(f, 512, stride=4), :]
        high = value.astype(BF16)
        rest = (value - high.astype(F32)).astype(BF16)
        both = jnp.concatenate([high, rest], axis=1)
        both = jnp.dot(hit_ref[...], both, preferred_element_type=F32)
        sum_ref[f] = both[:, :128] + both[:, 128:]

    def lay_out(f, a, yo, h):
        tiles = []
        for z in (0, 1):
            tiles.append([])
            for bh in (0, 1):
                t0 = (a * 4 + yo * 2 + bh) * 32 + (h * 2 + z) * 8
                tiles[z].append(sum_ref[f, pl.ds(t0, 8), :])
        blocks = tiles_to_grid(tiles, swaps)
        for u in range(4):
            at = (a * 4 + u, pl.ds(yo * 8, 8), pl.ds(h * 128, 128))
            add = blocks[u] * (1.0 / CELL_MASS)
            if f < 3:
                out_ref[f, *at] = base_ref[f, *at] + add
            else:
                out_ref[3, *at] = base_ref[3, *at] - LATENT_HEAT * add
                out_ref[4, *at] = base_ref[4, *at] + add

    order = (3, 0, 1, 2)
    add_up(order[0])
    for n, f in enumerate(order):
        if n < 3:
            add_up(order[n + 1])
        for a in range(4):
            for yo in (0, 1):
                for h in (0, 1):
                    lay_out(f, a, yo, h)
        for field in (3, 4) if f == 3 else (f,):
            store = pltpu.make_async_copy(out_ref.at[field], out_hbm.at[field], sems.at[2 + field])
            store.start()
            stores.append(store)
    for store in stores:
        store.wait()


VMEM = pl.BlockSpec(memory_space=pltpu.VMEM)
SMEM = pl.BlockSpec(memory_space=pltpu.SMEM)
HBM = pl.BlockSpec(memory_space=pltpu.HBM)


def call(kernel, name, out, in_specs, out_specs, scratch=(), limit=48, **params):
    return pl.pallas_call(
        kernel,
        name=name,
        out_shape=out,
        in_specs=in_specs,
        out_specs=out_specs,
        scratch_shapes=scratch,
        compiler_params=pltpu.CompilerParams(vmem_limit_bytes=limit * 1024 * 1024, **params),
    )


def array(*shape, dtype=F32):
    return jax.ShapeDtypeStruct(shape, dtype)


def shards(gas_state, parcel_speed, parcel_mass, offsets, cell_base, block_tile, block_count):
    def three(value):
        return value.reshape(DEVICES, 4, 3, 128).transpose(0, 2, 1, 3).reshape(SLOTS * 3, 128)

    def hbm(value):
        return pltpu.with_memory_space_constraint(value, pltpu.HBM)

    dma = pltpu.SemaphoreType.DMA
    parcel_outs = (array(SLOTS * 3, 128), array(SLOTS, 128))
    grid = array(*gas_state.shape)
    edge = (4, 5, 16, 256)
    speed_next, mass_next, arrived, wanted, base = call(
        exchange_kernel,
        "exchange",
        parcel_outs + (array(SLOTS * 4, 128), array(8, 128, dtype=I32), grid),
        [HBM] * 7,
        (VMEM,) * 5,
        [
            pltpu.VMEM(gas_state.shape, F32),
            pltpu.VMEM((SLOTS * 3, 128), F32),
            pltpu.VMEM((SLOTS, 128), F32),
            pltpu.VMEM((SLOTS * 3, 128), F32),
            pltpu.VMEM((SLOTS * 3, 128), I32),
            pltpu.SMEM((DEVICES,), I32),
            pltpu.VMEM((4, DEVICES), I32),
            pltpu.VMEM((DEVICES, 1, 128), I32),
            pltpu.VMEM((DEVICES, 1, 128), I32),
            pltpu.SMEM((DEVICES, 1, 128), I32),
            pltpu.VMEM((SLOTS, 4, 128), F32),
            pltpu.VMEM((SLOTS * 4, 128), F32),
            pltpu.VMEM((SLOTS * 4, 128), F32),
            pltpu.VMEM((SLOTS * 4, 128), F32),
            pltpu.VMEM((4, 256, 128), F32),
            pltpu.VMEM((4, 8, 128), I32),
            pltpu.VMEM(edge, F32),
            pltpu.VMEM(edge, F32),
            pltpu.SemaphoreType.REGULAR((4,)),
            dma((7,)),
            dma((5,)),
            dma((TURNS,)),
            dma((TURNS,)),
            dma((TURNS,)),
            dma((4,)),
            dma((4,)),
        ],
        limit=48,
        collective_id=0,
        has_side_effects=True,
    )(
        hbm(block_count.reshape(DEVICES)),
        hbm(block_tile.reshape(DEVICES, 4).T),
        hbm(gas_state),
        hbm(three(parcel_speed)),
        hbm(parcel_mass.reshape(SLOTS, 128)),
        hbm(three(offsets)),
        hbm(three(cell_base)),
    )
    gas_next, speed_next, mass_next = call(
        finish_kernel,
        "finish",
        (grid,) + parcel_outs,
        [VMEM] * 5,
        (HBM,) * 3,
        [
            pltpu.VMEM(gas_state.shape, F32),
            pltpu.VMEM((4, SLOTS, 128), F32),
            pltpu.VMEM((SLOTS, SLOTS), BF16),
            dma((7,)),
        ],
    )(base, wanted, arrived, speed_next, mass_next)
    speed_next = speed_next.reshape(DEVICES, 3, 4, 128).transpose(0, 2, 1, 3)
    return gas_next, speed_next.reshape(parcel_speed.shape), mass_next.reshape(parcel_mass.shape)


def solution(mesh):
    in_specs = (
        P(None, "gx", "yz", None),
        P("gx", "yz", None, None, None, None),
        P("gx", "yz", None, None, None),
        P("gx", "yz", None, None, None, None),
        P("gx", "yz", None, None, None, None),
        P("gx", "yz", None, None),
        P("gx", "yz", None),
    )
    out_specs = (
        P(None, "gx", "yz", None),
        P("gx", "yz", None, None, None, None),
        P("gx", "yz", None, None, None),
    )
    return jax.shard_map(shards, mesh=mesh, in_specs=in_specs, out_specs=out_specs, check_vma=False)
```
